32 devices in a mesh: replica: 8 (over y, x, core), tensor: 4 (over z).
Axes of the slice: x: 2, y: 2, z: 4, core: 2. Of those that a mesh axis runs over, the one named last changes fastest.
Arguments:
- weights: bfloat16 [8, 7168, 2048], P('replica', 'tensor'), may hold values from -6 to 6
- hidden: bfloat16 [8, 2, 512, 7168], P('replica', None, None, 'tensor'), may hold values from -6 to 6
- targets: bfloat16 [8, 2, 512, 2048], P('replica'), may hold values from -6 to 6
- norm_gain: float32 [2048], replicated, may hold values from 0.5 to 2
- stragglers: int32 [2, 8], replicated, may hold values 0 or 1
Outputs:
- new_weights: bfloat16 [8, 7168, 2048], P('replica', 'tensor')
The draws below stay inside these ranges and needn't reach their ends.
All inputs are finite; a program needn't handle non-finite values.
Results may differ from the reference program's by a relative error of at most 0.011.
Values may be sent and summed in bfloat16 or wider, within the bound.
A program may use at most 128 MiB of HBM per device.

```python
import math
import jax
import jax.numpy as jnp
from jax import lax

D = 2048
FF = 7168
TOK_DEV = 512
STEPS = 2
REPLICAS = 8
N_REPLICA = 8


def set_ends(entries, own_key, low, high):
    place = [jax.random.randint(jax.random.fold_in(own_key, axis), (), 0, length) for axis, length in enumerate(entries.shape)]
    widest = entries.shape.index(max(entries.shape))
    neighbour = place[:widest] + [(place[widest] + 1) % entries.shape[widest]] + place[widest + 1:]
    return entries.at[tuple(place)].set(low).at[tuple(neighbour)].set(high)


def block_levels(key, dims, shards, smallest, top_value):
    loudness, own = 1.0, jax.random.fold_in(key, 6)
    for position, blocks in shards:
        heights = jnp.exp(jax.random.uniform(jax.random.fold_in(own, position), (blocks,), jnp.float32, smallest / len(shards), top_value / len(shards)))
        loudness = loudness * jnp.repeat(heights, dims[position] // blocks).reshape([-1 if axis == position else 1 for axis in range(len(dims))])
    return loudness


def centred(rng, dims, spread, most, shards=(), held_as=jnp.bfloat16):
    factor_of = block_levels(rng, dims, shards, -0.22, 0.18) if shards else 1.0
    drawn = jax.random.normal(rng, dims, jnp.float32) * spread * factor_of
    return jnp.minimum(jnp.maximum(drawn, -most), most).astype(held_as)


def setup_inputs(seed: int = 0) -> dict:
    arg_keys = jax.random.split(jax.random.key(seed), 6)
    return {
        "weights": centred(arg_keys[0], (REPLICAS, FF, D), 1.0, 6.0, ((0, 8), (1, 4))),
        "hidden": centred(arg_keys[1], (REPLICAS, STEPS, TOK_DEV, FF), 1.0, 6.0, ((0, 8), (3, 4))),
        "targets": centred(arg_keys[2], (REPLICAS, STEPS, TOK_DEV, D), 1.0, 6.0, ((0, 8),)),
        "norm_gain": jnp.clip(jnp.exp(jax.random.uniform(arg_keys[3], (D,), jnp.float32, math.log(0.5), math.log(2.0))), 0.5, 2.0),
        "stragglers": set_ends((jax.random.randint(arg_keys[4], (STEPS, REPLICAS), 0, 4) < 1).astype(jnp.int32), jax.random.fold_in(arg_keys[4], 1), 0, 1),
    }


eps = 1e-05
learn_rate = 0.5

def contract_rows(left, right):
    return lax.dot_general(left, right, (((0,), (0,)), ((), ())), preferred_element_type=jnp.float32)

def norm_backward(outputs, target_rows, norm_gain):
    squares = lax.optimization_barrier(jnp.mean(outputs * outputs, axis=-1, keepdims=True))
    inverse = lax.rsqrt(squares + eps)
    normed = outputs * inverse
    weighted = (normed * norm_gain - target_rows.astype(jnp.float32)) * norm_gain
    cross_mean = lax.optimization_barrier(jnp.mean(weighted * normed, axis=-1, keepdims=True))
    return (inverse * (weighted - normed * cross_mean)).astype(jnp.bfloat16)

def local_update(weight_block, hidden_rows, target_rows, norm_gain):
    factor = FF ** (-0.5)
    outputs = factor * jnp.dot(hidden_rows, weight_block, preferred_element_type=jnp.float32)
    grad_out = norm_backward(outputs, target_rows, norm_gain)
    grad_weight = (factor * contract_rows(hidden_rows, grad_out)).astype(jnp.bfloat16)
    return (weight_block.astype(jnp.float32) - learn_rate * grad_weight.astype(jnp.float32)).astype(jnp.bfloat16)

def reference(weights, hidden, targets, norm_gain, stragglers):
    levels = N_REPLICA.bit_length() - 1
    indices = jnp.arange(N_REPLICA, dtype=jnp.int32)
    for update_step in range(STEPS):
        bit_index = update_step % levels
        updated = lax.map(lambda element: local_update(element[0], element[1], element[2], norm_gain), (weights, hidden[:, update_step], targets[:, update_step]))
        partner = jnp.bitwise_xor(indices, jnp.int32(1 << bit_index)).astype(jnp.int32)
        paired = updated[partner]
        mask_row = stragglers[update_step]
        keep_pair = (mask_row == 0) & (mask_row[partner] == 0)
        averaged = ((updated.astype(jnp.float32) + paired.astype(jnp.float32)) * 0.5).astype(jnp.bfloat16)
        weights = jnp.where(keep_pair[:, None, None], averaged, updated)
    return weights
```

```python
import functools

import jax
import jax.numpy as jnp
from jax import lax
from jax.experimental import pallas as pl
from jax.experimental.pallas import tpu as pltpu
from jax.sharding import PartitionSpec as P

eps = 1e-05
learn_rate = 0.5

MESH = pl.DeviceIdType.MESH
TILE = 512
ROWS = 128
SLAB = 128
MIDDLE = 4 / 14
EARLY = 3 / 14


def contract_rows(left, right):
    return lax.dot_general(
        left, right, (((0,), (0,)), ((), ())), preferred_element_type=jnp.float32
    )


def norm_backward(outputs, target_rows, norm_gain):
    squares = jnp.mean(outputs * outputs, axis=-1, keepdims=True)
    inverse = lax.rsqrt(squares + eps)
    normed = outputs * inverse
    weighted = (normed * norm_gain - target_rows.astype(jnp.float32)) * norm_gain
    cross_mean = jnp.mean(weighted * normed, axis=-1, keepdims=True)
    return (inverse * (weighted - normed * cross_mean)).astype(jnp.bfloat16)


def flip(index, bit):
    return index + bit - 2 * bit * ((index // bit) % 2)


def steps_kernel(middle, early, *refs):
    weights_ref, hidden_ref, targets_ref, gain_ref, late_ref, new_ref = refs[:6]
    own, theirs, far_own, crossed, rows_in, far_first, far_second = refs[6:13]
    goal, terms, arriving, out_right, out_left, grads, far_grads = refs[13:20]
    tile_load, load, right_send, right_recv, left_send, left_recv = refs[20:26]
    near_send, near_recv, cargo_send, cargo_recv, swap_send, swap_recv = refs[26:32]
    side_send, side_recv, across_send, across_recv = refs[32:36]
    share_right, share_left, share_recv, store_sem = refs[36:]

    count = lax.axis_size("tensor")
    me = lax.axis_index("tensor")
    replica = lax.axis_index("replica")
    last = count - 1
    near, far = flip(replica, 1), flip(replica, 2)
    cross = flip(near, 2)
    depth, features = own.shape
    tokens = grads.shape[1]
    tiles = terms.shape[0]
    blocks = tokens // ROWS
    chunks = tiles * blocks
    slabs = depth // SLAB
    ready = middle + early
    factor = (depth * count) ** (-0.5)

    def share_of(step, one, other):
        late = (late_ref[step, one] != 0) | (late_ref[step, other] != 0)
        return jnp.where(late, 1.0, 0.5), jnp.where(late, 0.0, 0.5)

    own_mix = share_of(0, replica, near)
    far_mix = share_of(0, far, cross)
    end_mix = share_of(1, replica, far)

    def mix(shares, one, other):
        return (
            one.astype(jnp.float32) * shares[0] + other.astype(jnp.float32) * shares[1]
        ).astype(jnp.bfloat16)

    def columns_of(tile):
        return pl.ds(pl.multiple_of(tile * TILE, TILE), TILE)

    def tile_copy(tile):
        span = columns_of(tile)
        return pltpu.make_async_copy(
            weights_ref.at[0, :, span], own.at[:, span], tile_load.at[tile]
        )

    def hidden_copy(step):
        return pltpu.make_async_copy(hidden_ref.at[0, step], rows_in.at[step], load.at[step, 0])

    def target_copy(step):
        return pltpu.make_async_copy(targets_ref.at[0, step], goal.at[step], load.at[step, 1])

    hidden_copy(0).start()
    for tile in range(tiles):
        tile_copy(tile).start()
    target_copy(0).start()
    hidden_copy(1).start()
    target_copy(1).start()

    barrier = pltpu.get_barrier_semaphore()
    pl.semaphore_signal(barrier, inc=1, device_id=(far, me), device_id_type=MESH)
    pl.semaphore_signal(barrier, inc=1, device_id=(near, me), device_id_type=MESH)
    for hop in range(1, count):
        peer = lax.rem(me + hop, count)
        pl.semaphore_signal(barrier, inc=1, device_id=(replica, peer), device_id_type=MESH)
    pl.semaphore_wait(barrier, count + 1)

    def slab_rows(slab):
        return pl.ds(pl.multiple_of(slab * SLAB, SLAB), SLAB)

    def remote(source, target, send, recv, device):
        return pltpu.make_async_remote_copy(
            src_ref=source, dst_ref=target, send_sem=send, recv_sem=recv,
            device_id=device, device_id_type=MESH,
        )

    def early_cargo(slab):
        span = slab_rows(slab)
        return remote(
            weights_ref.at[0, span], far_own.at[span],
            cargo_send.at[slab], cargo_recv.at[slab], (far, me),
        )

    def cargo(slab):
        span = slab_rows(slab)
        return remote(
            own.at[span], far_own.at[span],
            cargo_send.at[slab], cargo_recv.at[slab], (far, me),
        )

    def side(step):
        if step:
            span, target = pl.ds(0, ready * SLAB), far_second
        else:
            span, target = pl.ds(middle * SLAB, early * SLAB), far_first
        return remote(
            hidden_ref.at[0, step, :, span], target,
            side_send.at[step], side_recv.at[step], (far, me),
        )

    for slab in range(middle, ready):
        early_cargo(slab).start()
    for step in range(2):
        side(step).start()

    @pl.when(me == 0)
    def _():
        for step in range(2):
            arriving[step, 0] = jnp.zeros(arriving.shape[2:], arriving.dtype)

    @pl.when(me == last)
    def _():
        for step in range(2):
            arriving[step, 1] = jnp.zeros(arriving.shape[2:], arriving.dtype)

    def place(chunk):
        return chunk % tiles, pl.ds(pl.multiple_of((chunk // tiles) * ROWS, ROWS), ROWS)

    def right_copy(step, chunk):
        tile, rows = place(chunk)
        return remote(
            out_right.at[tile, rows], arriving.at[step, 0, tile, rows],
            right_send.at[step, chunk], right_recv.at[step, chunk],
            (replica, lax.rem(me + 1, count)),
        )

    def left_copy(step, chunk):
        tile, rows = place(chunk)
        return remote(
            out_left.at[tile, rows], arriving.at[step, 1, tile, rows],
            left_send.at[step, chunk], left_recv.at[step, chunk],
            (replica, lax.rem(me + count - 1, count)),
        )

    block = ROWS // tiles
    lag = tiles - 1 + jnp.maximum(me, last - me)

    def chain(step):
        def turn(now, _):
            @pl.when(now < chunks)
            def _():
                if step == 0:

                    @pl.when(now < tiles)
                    def _():
                        tile_copy(now).wait()

                tile, rows = place(now)
                terms[tile, rows, :] = factor * jnp.dot(
                    rows_in[step, rows, :], own[:, columns_of(tile)],
                    preferred_element_type=jnp.float32,
                )

            rightward = now - me

            @pl.when((rightward >= 0) & (rightward < chunks))
            def _():
                @pl.when(me > 0)
                def _():
                    right_copy(step, rightward).wait_recv()

                @pl.when(me < last)
                def _():
                    tile, rows = place(rightward)
                    total = terms[tile, rows, :] + arriving[step, 0, tile, rows, :].astype(jnp.float32)
                    out_right[tile, rows, :] = total.astype(jnp.bfloat16)
                    right_copy(step, rightward).start()

            leftward = now - (last - me)

            @pl.when((leftward >= 0) & (leftward < chunks))
            def _():
                @pl.when(me < last)
                def _():
                    left_copy(step, leftward).wait_recv()

                @pl.when(me > 0)
                def _():
                    tile, rows = place(leftward)
                    total = terms[tile, rows, :] + arriving[step, 1, tile, rows, :].astype(jnp.float32)
                    out_left[tile, rows, :] = total.astype(jnp.bfloat16)
                    left_copy(step, leftward).start()

            index = now - lag

            @pl.when((index >= 0) & (index < chunks))
            def _():
                @pl.when(index == 0)
                def _():
                    target_copy(step).wait()

                rows = pl.ds(pl.multiple_of(index * block, block), block)
                outputs = jnp.concatenate(
                    [
                        terms[tile, rows, :]
                        + arriving[step, 0, tile, rows, :].astype(jnp.float32)
                        + arriving[step, 1, tile, rows, :].astype(jnp.float32)
                        for tile in range(tiles)
                    ],
                    axis=1,
                )
                grads[step, rows, :] = norm_backward(outputs, goal[step, rows, :], gain_ref[...])

            return 0

        hidden_copy(step).wait()
        lax.fori_loop(0, chunks + tiles - 1 + last, turn, 0)

    def drain(step):
        def sent(chunk, _):
            @pl.when(me < last)
            def _():
                right_copy(step, chunk).wait_send()

            @pl.when(me > 0)
            def _():
                left_copy(step, chunk).wait_send()

            return 0

        lax.fori_loop(0, chunks, sent, 0)

    part = tokens // count

    def part_rows(index):
        return pl.ds(pl.multiple_of(index * part, part), part)

    def across(step):
        return remote(
            grads.at[step, part_rows(me)], far_grads.at[step, part_rows(me)],
            across_send.at[step], across_recv.at[step], (far, me),
        )

    def pass_right(step, index):
        piece = far_grads.at[step, part_rows(index)]
        return remote(
            piece, piece, share_right.at[step, index], share_recv.at[step, index],
            (replica, lax.rem(me + 1, count)),
        )

    def pass_left(step, index):
        piece = far_grads.at[step, part_rows(index)]
        return remote(
            piece, piece, share_left.at[step, index], share_recv.at[step, index],
            (replica, lax.rem(me + count - 1, count)),
        )

    def gather_first(step):
        across(step).wait_recv()

        @pl.when(me < last)
        def _():
            pass_right(step, me).start()

        @pl.when(me > 0)
        def _():
            pass_left(step, me).start()

    def gather_rest(step):
        def hop(distance, _):
            lower, upper = me - distance, me + distance

            @pl.when(lower >= 0)
            def _():
                pass_right(step, lower).wait_recv()

                @pl.when(me < last)
                def _():
                    pass_right(step, lower).start()

            @pl.when(upper <= last)
            def _():
                pass_left(step, upper).wait_recv()

                @pl.when(me > 0)
                def _():
                    pass_left(step, upper).start()

            return 0

        lax.fori_loop(1, count, hop, 0)

    def gather_sent(step):
        def hop(index, _):
            @pl.when((me < last) & (index <= me))
            def _():
                pass_right(step, index).wait_send()

            @pl.when((me > 0) & (index >= me))
            def _():
                pass_left(step, index).wait_send()

            return 0

        lax.fori_loop(0, count, hop, 0)

    def descended(block_rows, hidden_columns, gradient):
        grad_weight = (factor * contract_rows(hidden_columns, gradient)).astype(jnp.bfloat16)
        return (
            block_rows.astype(jnp.float32) - learn_rate * grad_weight.astype(jnp.float32)
        ).astype(jnp.bfloat16)

    def descend_own(step, slab):
        span = slab_rows(slab)
        own[span, :] = descended(own[span, :], rows_in[step, :, span], grads[step])

    def near_copy(slab):
        span = slab_rows(slab)
        return remote(
            own.at[span], theirs.at[span], near_send.at[slab], near_recv.at[slab], (near, me)
        )

    def swap(slab):
        index = slab - middle
        return remote(
            far_own.at[slab_rows(slab)], crossed.at[slab_rows(index)],
            swap_send.at[index], swap_recv.at[index], (near, me),
        )

    def store(slab):
        span = slab_rows(slab)
        return pltpu.make_async_copy(own.at[span], new_ref.at[span], store_sem.at[slab])

    def loop(low, high, body):
        def run(index, _):
            body(index)
            return 0

        lax.fori_loop(low, high, run, 0)

    chain(0)
    across(0).start()

    def offer(slab):
        descend_own(0, slab)
        near_copy(slab).start()

    def settle(slab):
        span = slab_rows(slab)
        near_copy(slab).wait()
        own[span, :] = mix(own_mix, own[span, :], theirs[span, :])

        @pl.when(slab < middle)
        def _():
            cargo(slab).start()

    loop(0, slabs, offer)
    loop(0, slabs, settle)
    drain(0)

    chain(1)
    across(1).start()
    gather_first(0)

    def give(slab):
        descend_own(1, slab)
        cargo(slab).start()

    loop(ready, slabs, give)
    gather_rest(0)

    def keep(slab):
        @pl.when(slab < middle)
        def _():
            cargo(slab).wait_send()

        descend_own(1, slab)

    loop(0, ready, keep)

    side(0).wait_recv()

    def replay(slab):
        span = slab_rows(slab)
        early_cargo(slab).wait_recv()
        far_own[span, :] = descended(
            far_own[span, :], far_first[:, slab_rows(slab - middle)], far_grads[0]
        )
        swap(slab).start()

    def level(slab):
        span = slab_rows(slab)
        swap(slab).wait()
        far_own[span, :] = mix(far_mix, far_own[span, :], crossed[slab_rows(slab - middle), :])

    loop(middle, ready, replay)
    loop(middle, ready, level)

    gather_first(1)
    gather_rest(1)
    side(1).wait_recv()

    def join(slab):
        span = slab_rows(slab)

        @pl.when(slab < middle)
        def _():
            cargo(slab).wait_recv()

        other = descended(far_own[span, :], far_second[:, span], far_grads[1])
        own[span, :] = mix(end_mix, own[span, :], other)
        store(slab).start()

    loop(0, ready, join)

    def finish(slab):
        span = slab_rows(slab)
        cargo(slab).wait()
        own[span, :] = mix(end_mix, own[span, :], far_own[span, :])
        store(slab).start()

    loop(ready, slabs, finish)

    drain(1)
    for step in range(2):
        gather_sent(step)
        across(step).wait_send()
        side(step).wait_send()
    for slab in range(middle, ready):
        early_cargo(slab).wait_send()
    loop(0, slabs, lambda slab: store(slab).wait())


def on_device(weights, hidden, targets, norm_gain, stragglers):
    _, depth, features = weights.shape
    tokens = hidden.shape[2]
    count = lax.axis_size("tensor")
    tiles = features // TILE
    chunks = tiles * (tokens // ROWS)
    slabs = depth // SLAB
    middle, early = round(slabs * MIDDLE), round(slabs * EARLY)
    anywhere = pl.BlockSpec(memory_space=pl.ANY)

    def buffer(*shape, dtype=jnp.bfloat16):
        return pltpu.VMEM(shape, dtype)

    def sems(*shape):
        return pltpu.SemaphoreType.DMA(shape)

    return pl.pallas_call(
        functools.partial(steps_kernel, middle, early),
        out_shape=jax.ShapeDtypeStruct((depth, features), weights.dtype),
        in_specs=[anywhere] * 3
        + [pl.BlockSpec(memory_space=pltpu.VMEM), pl.BlockSpec(memory_space=pltpu.SMEM)],
        out_specs=anywhere,
        scratch_shapes=[
            buffer(depth, features),
            buffer(depth, features),
            buffer(depth, features),
            buffer(early * SLAB, features),
            buffer(2, tokens, depth),
            buffer(tokens, early * SLAB),
            buffer(tokens, (middle + early) * SLAB),
            buffer(2, tokens, features),
            buffer(tiles, tokens, TILE, dtype=jnp.float32),
            buffer(2, 2, tiles, tokens, TILE),
            buffer(tiles, tokens, TILE),
            buffer(tiles, tokens, TILE),
            buffer(2, tokens, features),
            buffer(2, tokens, features),
            sems(tiles),
            sems(2, 2),
            *[sems(2, chunks)] * 4,
            *[sems(slabs)] * 4,
            *[sems(early)] * 2,
            *[sems(2)] * 4,
            *[sems(2, count)] * 3,
            sems(slabs),
        ],
        compiler_params=pltpu.CompilerParams(
            collective_id=0, has_side_effects=True, vmem_limit_bytes=63 << 20
        ),
    )(weights, hidden, targets, norm_gain[None], stragglers)[None]


def solution(mesh):
    placed = (
        P("replica", "tensor", None),
        P("replica", None, None, "tensor"),
        P("replica", None, None, None),
        P(),
        P(),
    )
    return jax.shard_map(
        on_device,
        mesh=mesh,
        in_specs=placed,
        out_specs=P("replica", "tensor", None),
        check_vma=False,
    )
```

```python
import functools

import jax
import jax.numpy as jnp
from jax import lax
from jax.experimental import pallas as pl
from jax.experimental.pallas import tpu as pltpu
from jax.sharding import PartitionSpec as P

eps = 1e-05
learn_rate = 0.5

MESH = pl.DeviceIdType.MESH
TILE = 512
ROWS = 64
LAG = 3
SLAB = 128
MIDDLE = 5 / 14
EARLY = 3 / 14


def contract_rows(left, right):
    return lax.dot_general(
        left, right, (((0,), (0,)), ((), ())), preferred_element_type=jnp.float32
    )


def norm_backward(outputs, target_rows, norm_gain):
    squares = jnp.mean(outputs * outputs, axis=-1, keepdims=True)
    inverse = lax.rsqrt(squares + eps)
    normed = outputs * inverse
    weighted = (normed * norm_gain - target_rows.astype(jnp.float32)) * norm_gain
    cross_mean = jnp.mean(weighted * normed, axis=-1, keepdims=True)
    return (inverse * (weighted - normed * cross_mean)).astype(jnp.bfloat16)


def flip(index, bit):
    return index + bit - 2 * bit * ((index // bit) % 2)


def steps_kernel(middle, early, *refs):
    weights_ref, hidden_ref, targets_ref, gain_ref, late_ref, new_ref = refs[:6]
    own, theirs, far_own, crossed, rows_in, far_first, far_second = refs[6:13]
    goal, terms, arriving, out_right, out_left, grads, far_grads = refs[13:20]
    tile_load, load, right_send, right_recv, left_send, left_recv = refs[20:26]
    near_send, near_recv, cargo_send, cargo_recv, swap_send, swap_recv = refs[26:32]
    side_send, side_recv, across_send, across_recv = refs[32:36]
    share_right, share_left, share_recv, store_sem = refs[36:]

    count = lax.axis_size("tensor")
    me = lax.axis_index("tensor")
    replica = lax.axis_index("replica")
    last = count - 1
    near, far = flip(replica, 1), flip(replica, 2)
    cross = flip(near, 2)
    depth, features = own.shape
    tokens = grads.shape[1]
    tiles = terms.shape[0]
    blocks = tokens // ROWS
    chunks = tiles * blocks
    slabs = depth // SLAB
    ready = middle + early
    factor = (depth * count) ** (-0.5)

    def share_of(step, one, other):
        late = (late_ref[step, one] != 0) | (late_ref[step, other] != 0)
        return jnp.where(late, 1.0, 0.5), jnp.where(late, 0.0, 0.5)

    own_mix = share_of(0, replica, near)
    far_mix = share_of(0, far, cross)
    end_mix = share_of(1, replica, far)

    def mix(shares, one, other):
        return (
            one.astype(jnp.float32) * shares[0] + other.astype(jnp.float32) * shares[1]
        ).astype(jnp.bfloat16)

    def columns_of(tile):
        return pl.ds(pl.multiple_of(tile * TILE, TILE), TILE)

    def tile_copy(tile):
        span = columns_of(tile)
        return pltpu.make_async_copy(
            weights_ref.at[0, :, span], own.at[:, span], tile_load.at[tile]
        )

    def hidden_copy(step):
        return pltpu.make_async_copy(hidden_ref.at[0, step], rows_in.at[step], load.at[step, 0])

    def target_copy(step):
        return pltpu.make_async_copy(targets_ref.at[0, step], goal.at[step], load.at[step, 1])

    hidden_copy(0).start()
    for tile in range(tiles):
        tile_copy(tile).start()
    target_copy(0).start()
    hidden_copy(1).start()
    target_copy(1).start()

    barrier = pltpu.get_barrier_semaphore()
    pl.semaphore_signal(barrier, inc=1, device_id=(far, me), device_id_type=MESH)
    pl.semaphore_signal(barrier, inc=1, device_id=(near, me), device_id_type=MESH)
    for hop in range(1, count):
        peer = lax.rem(me + hop, count)
        pl.semaphore_signal(barrier, inc=1, device_id=(replica, peer), device_id_type=MESH)
    pl.semaphore_wait(barrier, count + 1)

    def slab_rows(slab):
        return pl.ds(pl.multiple_of(slab * SLAB, SLAB), SLAB)

    def remote(source, target, send, recv, device):
        return pltpu.make_async_remote_copy(
            src_ref=source, dst_ref=target, send_sem=send, recv_sem=recv,
            device_id=device, device_id_type=MESH,
        )

    def early_cargo(slab):
        span = slab_rows(slab)
        return remote(
            weights_ref.at[0, span], far_own.at[span],
            cargo_send.at[slab], cargo_recv.at[slab], (far, me),
        )

    def cargo(slab):
        span = slab_rows(slab)
        return remote(
            own.at[span], far_own.at[span],
            cargo_send.at[slab], cargo_recv.at[slab], (far, me),
        )

    def side(step):
        if step:
            span, target = pl.ds(0, ready * SLAB), far_second
        else:
            span, target = pl.ds(middle * SLAB, early * SLAB), far_first
        return remote(
            hidden_ref.at[0, step, :, span], target,
            side_send.at[step], side_recv.at[step], (far, me),
        )

    for slab in range(middle, ready):
        early_cargo(slab).start()
    for step in range(2):
        side(step).start()

    @pl.when(me == 0)
    def _():
        for step in range(2):
            arriving[step, 0] = jnp.zeros(arriving.shape[2:], arriving.dtype)

    @pl.when(me == last)
    def _():
        for step in range(2):
            arriving[step, 1] = jnp.zeros(arriving.shape[2:], arriving.dtype)

    def place(chunk):
        return chunk % tiles, pl.ds(pl.multiple_of((chunk // tiles) * ROWS, ROWS), ROWS)

    def right_copy(step, chunk):
        tile, rows = place(chunk)
        return remote(
            out_right.at[tile, rows], arriving.at[step, 0, tile, rows],
            right_send.at[step, chunk], right_recv.at[step, chunk],
            (replica, lax.rem(me + 1, count)),
        )

    def left_copy(step, chunk):
        tile, rows = place(chunk)
        return remote(
            out_left.at[tile, rows], arriving.at[step, 1, tile, rows],
            left_send.at[step, chunk], left_recv.at[step, chunk],
            (replica, lax.rem(me + count - 1, count)),
        )

    block = ROWS // tiles
    lag = tiles - 1 + LAG * jnp.maximum(me, last - me)

    def chain(step):
        def turn(now, _):
            @pl.when(now < chunks)
            def _():
                if step == 0:

                    @pl.when(now < tiles)
                    def _():
                        tile_copy(now).wait()

                tile, rows = place(now)
                terms[tile, rows, :] = factor * jnp.dot(
                    rows_in[step, rows, :], own[:, columns_of(tile)],
                    preferred_element_type=jnp.float32,
                )

            rightward = now - LAG * me

            @pl.when((rightward >= 0) & (rightward < chunks))
            def _():
                @pl.when(me > 0)
                def _():
                    right_copy(step, rightward).wait_recv()

                @pl.when(me < last)
                def _():
                    tile, rows = place(rightward)
                    total = terms[tile, rows, :] + arriving[step, 0, tile, rows, :].astype(jnp.float32)
                    out_right[tile, rows, :] = total.astype(jnp.bfloat16)
                    right_copy(step, rightward).start()

            leftward = now - LAG * (last - me)

            @pl.when((leftward >= 0) & (leftward < chunks))
            def _():
                @pl.when(me < last)
                def _():
                    left_copy(step, leftward).wait_recv()

                @pl.when(me > 0)
                def _():
                    tile, rows = place(leftward)
                    total = terms[tile, rows, :] + arriving[step, 1, tile, rows, :].astype(jnp.float32)
                    out_left[tile, rows, :] = total.astype(jnp.bfloat16)
                    left_copy(step, leftward).start()

            index = now - lag

            @pl.when((index >= 0) & (index < chunks))
            def _():
                @pl.when(index == 0)
                def _():
                    target_copy(step).wait()

                rows = pl.ds(pl.multiple_of(index * block, block), block)
                outputs = jnp.concatenate(
                    [
                        terms[tile, rows, :]
                        + arriving[step, 0, tile, rows, :].astype(jnp.float32)
                        + arriving[step, 1, tile, rows, :].astype(jnp.float32)
                        for tile in range(tiles)
                    ],
                    axis=1,
                )
                grads[step, rows, :] = norm_backward(outputs, goal[step, rows, :], gain_ref[...])

            return 0

        hidden_copy(step).wait()
        lax.fori_loop(0, chunks + tiles - 1 + LAG * last, turn, 0)

    def drain(step):
        def sent(chunk, _):
            @pl.when(me < last)
            def _():
                right_copy(step, chunk).wait_send()

            @pl.when(me > 0)
            def _():
                left_copy(step, chunk).wait_send()

            return 0

        lax.fori_loop(0, chunks, sent, 0)

    part = tokens // count

    def part_rows(index):
        return pl.ds(pl.multiple_of(index * part, part), part)

    def across(step):
        return remote(
            grads.at[step, part_rows(me)], far_grads.at[step, part_rows(me)],
            across_send.at[step], across_recv.at[step], (far, me),
        )

    def pass_right(step, index):
        piece = far_grads.at[step, part_rows(index)]
        return remote(
            piece, piece, share_right.at[step, index], share_recv.at[step, index],
            (replica, lax.rem(me + 1, count)),
        )

    def pass_left(step, index):
        piece = far_grads.at[step, part_rows(index)]
        return remote(
            piece, piece, share_left.at[step, index], share_recv.at[step, index],
            (replica, lax.rem(me + count - 1, count)),
        )

    def gather_first(step):
        across(step).wait_recv()

        @pl.when(me < last)
        def _():
            pass_right(step, me).start()

        @pl.when(me > 0)
        def _():
            pass_left(step, me).start()

    def gather_rest(step):
        def hop(distance, _):
            lower, upper = me - distance, me + distance

            @pl.when(lower >= 0)
            def _():
                pass_right(step, lower).wait_recv()

                @pl.when(me < last)
                def _():
                    pass_right(step, lower).start()

            @pl.when(upper <= last)
            def _():
                pass_left(step, upper).wait_recv()

                @pl.when(me > 0)
                def _():
                    pass_left(step, upper).start()

            return 0

        lax.fori_loop(1, count, hop, 0)

    def gather_sent(step):
        def hop(index, _):
            @pl.when((me < last) & (index <= me))
            def _():
                pass_right(step, index).wait_send()

            @pl.when((me > 0) & (index >= me))
            def _():
                pass_left(step, index).wait_send()

            return 0

        lax.fori_loop(0, count, hop, 0)

    def descended(block_rows, hidden_columns, gradient):
        grad_weight = (factor * contract_rows(hidden_columns, gradient)).astype(jnp.bfloat16)
        return (
            block_rows.astype(jnp.float32) - learn_rate * grad_weight.astype(jnp.float32)
        ).astype(jnp.bfloat16)

    def descend_own(step, slab):
        span = slab_rows(slab)
        own[span, :] = descended(own[span, :], rows_in[step, :, span], grads[step])

    def near_copy(slab):
        span = slab_rows(slab)
        return remote(
            own.at[span], theirs.at[span], near_send.at[slab], near_recv.at[slab], (near, me)
        )

    def swap(slab):
        index = slab - middle
        return remote(
            far_own.at[slab_rows(slab)], crossed.at[slab_rows(index)],
            swap_send.at[index], swap_recv.at[index], (near, me),
        )

    def store(slab):
        span = slab_rows(slab)
        return pltpu.make_async_copy(own.at[span], new_ref.at[span], store_sem.at[slab])

    def loop(low, high, body):
        def run(index, _):
            body(index)
            return 0

        lax.fori_loop(low, high, run, 0)

    chain(0)
    across(0).start()

    def offer(slab):
        descend_own(0, slab)
        near_copy(slab).start()

    def settle(slab):
        span = slab_rows(slab)
        near_copy(slab).wait()
        own[span, :] = mix(own_mix, own[span, :], theirs[span, :])

        @pl.when(slab < middle)
        def _():
            cargo(slab).start()

    loop(0, slabs, offer)
    loop(0, slabs, settle)
    drain(0)

    chain(1)
    across(1).start()
    gather_first(0)

    def give(slab):
        descend_own(1, slab)
        cargo(slab).start()

    loop(ready, slabs, give)
    gather_first(1)
    gather_rest(0)

    def keep(slab):
        @pl.when(slab < middle)
        def _():
            cargo(slab).wait_send()

        descend_own(1, slab)

    loop(0, ready, keep)

    side(0).wait_recv()

    def replay(slab):
        span = slab_rows(slab)
        early_cargo(slab).wait_recv()
        far_own[span, :] = descended(
            far_own[span, :], far_first[:, slab_rows(slab - middle)], far_grads[0]
        )
        swap(slab).start()

    def level(slab):
        span = slab_rows(slab)
        swap(slab).wait()
        far_own[span, :] = mix(far_mix, far_own[span, :], crossed[slab_rows(slab - middle), :])

    loop(middle, ready, replay)
    loop(middle, ready, level)
    gather_rest(1)
    side(1).wait_recv()

    def join(slab):
        span = slab_rows(slab)

        @pl.when(slab < middle)
        def _():
            cargo(slab).wait_recv()

        other = descended(far_own[span, :], far_second[:, span], far_grads[1])
        own[span, :] = mix(end_mix, own[span, :], other)
        store(slab).start()

    loop(0, ready, join)

    def finish(slab):
        span = slab_rows(slab)
        cargo(slab).wait()
        own[span, :] = mix(end_mix, own[span, :], far_own[span, :])
        store(slab).start()

    loop(ready, slabs, finish)

    drain(1)
    for step in range(2):
        gather_sent(step)
        across(step).wait_send()
        side(step).wait_send()
    for slab in range(middle, ready):
        early_cargo(slab).wait_send()
    loop(0, slabs, lambda slab: store(slab).wait())


def on_device(weights, hidden, targets, norm_gain, stragglers):
    _, depth, features = weights.shape
    tokens = hidden.shape[2]
    count = lax.axis_size("tensor")
    tiles = features // TILE
    chunks = tiles * (tokens // ROWS)
    slabs = depth // SLAB
    middle, early = round(slabs * MIDDLE), round(slabs * EARLY)
    anywhere = pl.BlockSpec(memory_space=pl.ANY)

    def buffer(*shape, dtype=jnp.bfloat16):
        return pltpu.VMEM(shape, dtype)

    def sems(*shape):
        return pltpu.SemaphoreType.DMA(shape)

    return pl.pallas_call(
        functools.partial(steps_kernel, middle, early),
        out_shape=jax.ShapeDtypeStruct((depth, features), weights.dtype),
        in_specs=[anywhere] * 3
        + [pl.BlockSpec(memory_space=pltpu.VMEM), pl.BlockSpec(memory_space=pltpu.SMEM)],
        out_specs=anywhere,
        scratch_shapes=[
            buffer(depth, features),
            buffer(depth, features),
            buffer(depth, features),
            buffer(early * SLAB, features),
            buffer(2, tokens, depth),
            buffer(tokens, early * SLAB),
            buffer(tokens, (middle + early) * SLAB),
            buffer(2, tokens, features),
            buffer(tiles, tokens, TILE, dtype=jnp.float32),
            buffer(2, 2, tiles, tokens, TILE),
            buffer(tiles, tokens, TILE),
            buffer(tiles, tokens, TILE),
            buffer(2, tokens, features),
            buffer(2, tokens, features),
            sems(tiles),
            sems(2, 2),
            *[sems(2, chunks)] * 4,
            *[sems(slabs)] * 4,
            *[sems(early)] * 2,
            *[sems(2)] * 4,
            *[sems(2, count)] * 3,
            sems(slabs),
        ],
        compiler_params=pltpu.CompilerParams(
            collective_id=0, has_side_effects=True, vmem_limit_bytes=63 << 20
        ),
    )(weights, hidden, targets, norm_gain[None], stragglers)[None]


def solution(mesh):
    placed = (
        P("replica", "tensor", None),
        P("replica", None, None, "tensor"),
        P("replica", None, None, None),
        P(),
        P(),
    )
    return jax.shard_map(
        on_device,
        mesh=mesh,
        in_specs=placed,
        out_specs=P("replica", "tensor", None),
        check_vma=False,
    )
```

```python
import functools

import jax
import jax.numpy as jnp
from jax import lax
from jax.experimental import pallas as pl
from jax.experimental.pallas import tpu as pltpu
from jax.sharding import PartitionSpec as P

eps = 1e-05
learn_rate = 0.5

MESH = pl.DeviceIdType.MESH
TILE = 512
ROWS = 64
LAG = 3
SLAB = 128
PAIR = 1
MIDDLE = 5 / 14
EARLY = 3 / 14


def contract_rows(left, right):
    return lax.dot_general(
        left, right, (((0,), (0,)), ((), ())), preferred_element_type=jnp.float32
    )


def norm_backward(outputs, target_rows, norm_gain):
    squares = jnp.mean(outputs * outputs, axis=-1, keepdims=True)
    inverse = lax.rsqrt(squares + eps)
    normed = outputs * inverse
    weighted = (normed * norm_gain - target_rows.astype(jnp.float32)) * norm_gain
    cross_mean = jnp.mean(weighted * normed, axis=-1, keepdims=True)
    return (inverse * (weighted - normed * cross_mean)).astype(jnp.bfloat16)


def flip(index, bit):
    return index + bit - 2 * bit * ((index // bit) % 2)


def steps_kernel(middle, early, *refs):
    weights_ref, hidden_ref, targets_ref, gain_ref, late_ref, own = refs[:6]
    theirs, far_own, crossed, rows_in, far_first, far_second = refs[6:12]
    goal, terms, arriving, out_right, out_left, grads, far_grads = refs[12:19]
    tile_load, load, right_send, right_recv, left_send, left_recv = refs[19:25]
    near_send, near_recv, cargo_send, cargo_recv, swap_send, swap_recv = refs[25:31]
    side_send, side_recv, across_send, across_recv = refs[31:35]
    share_right, share_left, share_recv = refs[35:]

    count = lax.axis_size("tensor")
    me = lax.axis_index("tensor")
    replica = lax.axis_index("replica")
    last = count - 1
    near, far = flip(replica, 1), flip(replica, 2)
    cross = flip(near, 2)
    depth, features = own.shape
    tokens = grads.shape[1]
    tiles = terms.shape[0]
    blocks = tokens // ROWS
    chunks = tiles * blocks
    slabs = depth // SLAB
    ready = middle + early
    factor = (depth * count) ** (-0.5)

    def share_of(step, one, other):
        late = (late_ref[step, one] != 0) | (late_ref[step, other] != 0)
        return jnp.where(late, 1.0, 0.5), jnp.where(late, 0.0, 0.5)

    own_mix = share_of(0, replica, near)
    far_mix = share_of(0, far, cross)
    end_mix = share_of(1, replica, far)

    def mix(shares, one, other):
        return (
            one.astype(jnp.float32) * shares[0] + other.astype(jnp.float32) * shares[1]
        ).astype(jnp.bfloat16)

    def columns_of(tile):
        return pl.ds(pl.multiple_of(tile * TILE, TILE), TILE)

    def tile_copy(tile):
        span = columns_of(tile)
        return pltpu.make_async_copy(
            weights_ref.at[0, :, span], own.at[:, span], tile_load.at[tile]
        )

    def hidden_copy(step):
        return pltpu.make_async_copy(hidden_ref.at[0, step], rows_in.at[step], load.at[step, 0])

    def target_copy(step):
        return pltpu.make_async_copy(targets_ref.at[0, step], goal.at[step], load.at[step, 1])

    hidden_copy(0).start()
    for tile in range(tiles):
        tile_copy(tile).start()
    target_copy(0).start()
    hidden_copy(1).start()
    target_copy(1).start()

    barrier = pltpu.get_barrier_semaphore()
    pl.semaphore_signal(barrier, inc=1, device_id=(far, me), device_id_type=MESH)
    pl.semaphore_signal(barrier, inc=1, device_id=(near, me), device_id_type=MESH)

    @pl.when(me > 0)
    def _():
        pl.semaphore_signal(barrier, inc=1, device_id=(replica, me - 1), device_id_type=MESH)

    @pl.when(me < last)
    def _():
        pl.semaphore_signal(barrier, inc=1, device_id=(replica, me + 1), device_id_type=MESH)

    ends = jnp.where((me == 0) | (me == last), 1, 2)
    pl.semaphore_wait(barrier, 2 + ends)

    def slab_rows(slab):
        return pl.ds(pl.multiple_of(slab * SLAB, SLAB), SLAB)

    def remote(source, target, send, recv, device):
        return pltpu.make_async_remote_copy(
            src_ref=source, dst_ref=target, send_sem=send, recv_sem=recv,
            device_id=device, device_id_type=MESH,
        )

    def early_cargo(slab):
        span = slab_rows(slab)
        return remote(
            weights_ref.at[0, span], far_own.at[span],
            cargo_send.at[slab], cargo_recv.at[slab], (far, me),
        )

    def cargo(slab):
        span = slab_rows(slab)
        return remote(
            own.at[span], far_own.at[span],
            cargo_send.at[slab], cargo_recv.at[slab], (far, me),
        )

    def side(step):
        if step:
            span, target = pl.ds(0, ready * SLAB), far_second
        else:
            span, target = pl.ds(middle * SLAB, early * SLAB), far_first
        return remote(
            hidden_ref.at[0, step, :, span], target,
            side_send.at[step], side_recv.at[step], (far, me),
        )

    for slab in range(middle, ready):
        early_cargo(slab).start()
    for step in range(2):
        side(step).start()

    @pl.when(me == 0)
    def _():
        for step in range(2):
            arriving[step, 0] = jnp.zeros(arriving.shape[2:], arriving.dtype)

    @pl.when(me == last)
    def _():
        for step in range(2):
            arriving[step, 1] = jnp.zeros(arriving.shape[2:], arriving.dtype)

    def place(chunk):
        return chunk % tiles, pl.ds(pl.multiple_of((chunk // tiles) * ROWS, ROWS), ROWS)

    def right_copy(step, chunk):
        tile, rows = place(chunk)
        return remote(
            out_right.at[tile, rows], arriving.at[step, 0, tile, rows],
            right_send.at[step], right_recv.at[chunk],
            (replica, lax.rem(me + 1, count)),
        )

    def left_copy(step, chunk):
        tile, rows = place(chunk)
        return remote(
            out_left.at[tile, rows], arriving.at[step, 1, tile, rows],
            left_send.at[step], left_recv.at[chunk],
            (replica, lax.rem(me + count - 1, count)),
        )

    block = ROWS // tiles
    lag = tiles - 1 + LAG * jnp.maximum(me, last - me)

    def chain(step):
        def turn(now, _):
            @pl.when(now < chunks)
            def _():
                if step == 0:

                    @pl.when(now < tiles)
                    def _():
                        tile_copy(now).wait()

                tile, rows = place(now)
                terms[tile, rows, :] = factor * jnp.dot(
                    rows_in[step, rows, :], own[:, columns_of(tile)],
                    preferred_element_type=jnp.float32,
                )

            rightward = now - LAG * me

            @pl.when((rightward >= 0) & (rightward < chunks))
            def _():
                @pl.when(me > 0)
                def _():
                    right_copy(step, rightward).wait_recv()

                @pl.when(me < last)
                def _():
                    tile, rows = place(rightward)
                    total = terms[tile, rows, :] + arriving[step, 0, tile, rows, :].astype(jnp.float32)
                    out_right[tile, rows, :] = total.astype(jnp.bfloat16)
                    right_copy(step, rightward).start()

            leftward = now - LAG * (last - me)

            @pl.when((leftward >= 0) & (leftward < chunks))
            def _():
                @pl.when(me < last)
                def _():
                    left_copy(step, leftward).wait_recv()

                @pl.when(me > 0)
                def _():
                    tile, rows = place(leftward)
                    total = terms[tile, rows, :] + arriving[step, 1, tile, rows, :].astype(jnp.float32)
                    out_left[tile, rows, :] = total.astype(jnp.bfloat16)
                    left_copy(step, leftward).start()

            index = now - lag

            @pl.when((index >= 0) & (index < chunks))
            def _():
                @pl.when(index == 0)
                def _():
                    target_copy(step).wait()

                rows = pl.ds(pl.multiple_of(index * block, block), block)
                outputs = jnp.concatenate(
                    [
                        terms[tile, rows, :]
                        + arriving[step, 0, tile, rows, :].astype(jnp.float32)
                        + arriving[step, 1, tile, rows, :].astype(jnp.float32)
                        for tile in range(tiles)
                    ],
                    axis=1,
                )
                grads[step, rows, :] = norm_backward(outputs, goal[step, rows, :], gain_ref[...])

            return 0

        hidden_copy(step).wait()
        lax.fori_loop(0, chunks + tiles - 1 + LAG * last, turn, 0)

    def drain(step):
        @pl.when(me < last)
        def _():
            remote(
                out_right, arriving.at[step, 0], right_send.at[step], right_recv.at[0],
                (replica, lax.rem(me + 1, count)),
            ).wait_send()

        @pl.when(me > 0)
        def _():
            remote(
                out_left, arriving.at[step, 1], left_send.at[step], left_recv.at[0],
                (replica, lax.rem(me + count - 1, count)),
            ).wait_send()

    part = tokens // count

    def part_rows(index):
        return pl.ds(pl.multiple_of(index * part, part), part)

    def across(step):
        return remote(
            grads.at[step, part_rows(me)], far_grads.at[step, part_rows(me)],
            across_send.at[step], across_recv.at[step], (far, me),
        )

    def pass_right(step, index):
        piece = far_grads.at[step, part_rows(index)]
        return remote(
            piece, piece, share_right.at[step, index], share_recv.at[step, index],
            (replica, lax.rem(me + 1, count)),
        )

    def pass_left(step, index):
        piece = far_grads.at[step, part_rows(index)]
        return remote(
            piece, piece, share_left.at[step, index], share_recv.at[step, index],
            (replica, lax.rem(me + count - 1, count)),
        )

    def gather_first(step):
        across(step).wait_recv()

        @pl.when(me < last)
        def _():
            pass_right(step, me).start()

        @pl.when(me > 0)
        def _():
            pass_left(step, me).start()

    def gather_rest(step, low, high):
        def hop(distance, _):
            lower, upper = me - distance, me + distance

            @pl.when(lower >= 0)
            def _():
                pass_right(step, lower).wait_recv()

                @pl.when(me < last)
                def _():
                    pass_right(step, lower).start()

            @pl.when(upper <= last)
            def _():
                pass_left(step, upper).wait_recv()

                @pl.when(me > 0)
                def _():
                    pass_left(step, upper).start()

            return 0

        lax.fori_loop(low, high, hop, 0)

    def gather_sent(step):
        def hop(index, _):
            @pl.when((me < last) & (index <= me))
            def _():
                pass_right(step, index).wait_send()

            @pl.when((me > 0) & (index >= me))
            def _():
                pass_left(step, index).wait_send()

            return 0

        lax.fori_loop(0, count, hop, 0)

    def descended(block_rows, hidden_columns, gradient):
        grad_weight = (factor * contract_rows(hidden_columns, gradient)).astype(jnp.bfloat16)
        return (
            block_rows.astype(jnp.float32) - learn_rate * grad_weight.astype(jnp.float32)
        ).astype(jnp.bfloat16)

    def descend_own(step, span):
        own[span, :] = descended(own[span, :], rows_in[step, :, span], grads[step])

    def pair_rows(pair):
        return pl.ds(pl.multiple_of(pair * PAIR * SLAB, PAIR * SLAB), PAIR * SLAB)

    def near_copy(pair):
        span = pair_rows(pair)
        return remote(
            own.at[span], theirs.at[span], near_send.at[pair], near_recv.at[pair], (near, me)
        )

    def swap(slab):
        index = slab - middle
        return remote(
            far_own.at[slab_rows(slab)], crossed.at[slab_rows(index)],
            swap_send.at[index], swap_recv.at[index], (near, me),
        )

    def loop(low, high, body):
        def run(index, _):
            body(index)
            return 0

        lax.fori_loop(low, high, run, 0)

    chain(0)
    across(0).start()

    def offer(pair):
        descend_own(0, pair_rows(pair))
        near_copy(pair).start()

    def settle(pair):
        span = pair_rows(pair)
        near_copy(pair).wait()
        own[span, :] = mix(own_mix, own[span, :], theirs[span, :])
        for index in range(PAIR):
            slab = pair * PAIR + index

            @pl.when(slab < middle)
            def _():
                cargo(slab).start()

    loop(0, slabs // PAIR, offer)
    loop(0, slabs // PAIR, settle)
    drain(0)

    chain(1)
    across(1).start()
    gather_first(0)

    def give(slab):
        descend_own(1, slab_rows(slab))
        cargo(slab).start()

    loop(ready, slabs, give)
    gather_rest(0, 1, 2)
    gather_first(1)
    gather_rest(0, 2, count)

    def keep(slab):
        @pl.when(slab < middle)
        def _():
            cargo(slab).wait_send()

        descend_own(1, slab_rows(slab))

    loop(0, ready, keep)

    side(0).wait_recv()

    def replay(slab):
        span = slab_rows(slab)
        early_cargo(slab).wait_recv()
        far_own[span, :] = descended(
            far_own[span, :], far_first[:, slab_rows(slab - middle)], far_grads[0]
        )
        swap(slab).start()

    def level(slab):
        span = slab_rows(slab)
        swap(slab).wait()
        far_own[span, :] = mix(far_mix, far_own[span, :], crossed[slab_rows(slab - middle), :])

    loop(middle, ready, replay)
    loop(middle, ready, level)
    gather_rest(1, 1, count)
    side(1).wait_recv()

    def join(slab):
        span = slab_rows(slab)

        @pl.when(slab < middle)
        def _():
            cargo(slab).wait_recv()

        other = descended(far_own[span, :], far_second[:, span], far_grads[1])
        own[span, :] = mix(end_mix, own[span, :], other)

    loop(0, ready, join)

    def finish(slab):
        span = slab_rows(slab)
        cargo(slab).wait()
        own[span, :] = mix(end_mix, own[span, :], far_own[span, :])

    loop(ready, slabs, finish)

    drain(1)
    for step in range(2):
        gather_sent(step)
        across(step).wait_send()
        side(step).wait_send()
    for slab in range(middle, ready):
        early_cargo(slab).wait_send()


def on_device(weights, hidden, targets, norm_gain, stragglers):
    _, depth, features = weights.shape
    tokens = hidden.shape[2]
    count = lax.axis_size("tensor")
    tiles = features // TILE
    chunks = tiles * (tokens // ROWS)
    slabs = depth // SLAB
    middle, early = round(slabs * MIDDLE), round(slabs * EARLY)
    anywhere = pl.BlockSpec(memory_space=pl.ANY)

    def buffer(*shape, dtype=jnp.bfloat16):
        return pltpu.VMEM(shape, dtype)

    def sems(*shape):
        return pltpu.SemaphoreType.DMA(shape)

    return pl.pallas_call(
        functools.partial(steps_kernel, middle, early),
        out_shape=pltpu.VMEM((depth, features), weights.dtype),
        in_specs=[anywhere] * 3
        + [pl.BlockSpec(memory_space=pltpu.VMEM), pl.BlockSpec(memory_space=pltpu.SMEM)],
        out_specs=pl.BlockSpec(memory_space=pltpu.VMEM),
        scratch_shapes=[
            buffer(depth, features),
            buffer(depth, features),
            buffer(early * SLAB, features),
            buffer(2, tokens, depth),
            buffer(tokens, early * SLAB),
            buffer(tokens, (middle + early) * SLAB),
            buffer(2, tokens, features),
            buffer(tiles, tokens, TILE, dtype=jnp.float32),
            buffer(2, 2, tiles, tokens, TILE),
            buffer(tiles, tokens, TILE),
            buffer(tiles, tokens, TILE),
            buffer(2, tokens, features),
            buffer(2, tokens, features),
            sems(tiles),
            sems(2, 2),
            sems(2),
            sems(chunks),
            sems(2),
            sems(chunks),
            *[sems(slabs // PAIR)] * 2,
            *[sems(slabs)] * 2,
            *[sems(early)] * 2,
            *[sems(2)] * 4,
            *[sems(2, count)] * 3,
        ],
        compiler_params=pltpu.CompilerParams(
            collective_id=0, has_side_effects=True, vmem_limit_bytes=56 << 20
        ),
    )(weights, hidden, targets, norm_gain[None], stragglers)[None]


def solution(mesh):
    placed = (
        P("replica", "tensor", None),
        P("replica", None, None, "tensor"),
        P("replica", None, None, None),
        P(),
        P(),
    )
    return jax.shard_map(
        on_device,
        mesh=mesh,
        in_specs=placed,
        out_specs=P("replica", "tensor", None),
        check_vma=False,
    )
```

```python
import functools

import jax
import jax.numpy as jnp
from jax import lax
from jax.experimental import pallas as pl
from jax.experimental.pallas import tpu as pltpu
from jax.sharding import PartitionSpec as P

eps = 1e-05
learn_rate = 0.5

MESH = pl.DeviceIdType.MESH
TILE = 512
ROWS = 64
LAG = (3, 5)
SLAB = 128
PAIR = 1
EARLY = 3 / 14
MIDDLE = (0 / 14, 6 / 14)
YIELD = 36


def contract_rows(left, right):
    return lax.dot_general(
        left, right, (((0,), (0,)), ((), ())), preferred_element_type=jnp.float32
    )


def norm_backward(outputs, target_rows, norm_gain):
    squares = jnp.mean(outputs * outputs, axis=-1, keepdims=True)
    inverse = lax.rsqrt(squares + eps)
    normed = outputs * inverse
    weighted = (normed * norm_gain - target_rows.astype(jnp.float32)) * norm_gain
    cross_mean = jnp.mean(weighted * normed, axis=-1, keepdims=True)
    return (inverse * (weighted - normed * cross_mean)).astype(jnp.bfloat16)


def flip(index, bit):
    return index + bit - 2 * bit * ((index // bit) % 2)


def steps_kernel(early, middles, *refs):
    weights_ref, hidden_ref, targets_ref, gain_ref, late_ref, own = refs[:6]
    theirs, far_own, crossed, rows_in, far_first, far_second = refs[6:12]
    goal, terms, arriving, out_right, out_left, grads, far_grads = refs[12:19]
    tile_load, load, right_send, right_recv, left_send, left_recv = refs[19:25]
    near_send, near_recv, cargo_send, cargo_recv, swap_send, swap_recv = refs[25:31]
    side_send, side_recv, across_send, across_recv = refs[31:35]
    share_right, share_left, share_recv, turn_sem = refs[35:]

    count = lax.axis_size("tensor")
    me = lax.axis_index("tensor")
    replica = lax.axis_index("replica")
    last = count - 1
    near, far = flip(replica, 1), flip(replica, 2)
    cross = flip(near, 2)
    depth, features = own.shape
    tokens = grads.shape[1]
    tiles = terms.shape[0]
    blocks = tokens // ROWS
    chunks = tiles * blocks
    slabs = depth // SLAB
    parity = replica % 2
    least, most = early + middles[0], early + middles[1]
    ready = least + (most - least) * parity
    factor = (depth * count) ** (-0.5)

    def share_of(step, one, other):
        late = (late_ref[step, one] != 0) | (late_ref[step, other] != 0)
        return jnp.where(late, 1.0, 0.5), jnp.where(late, 0.0, 0.5)

    own_mix = share_of(0, replica, near)
    far_mix = share_of(0, far, cross)
    end_mix = share_of(1, replica, far)

    def mix(shares, one, other):
        return (
            one.astype(jnp.float32) * shares[0] + other.astype(jnp.float32) * shares[1]
        ).astype(jnp.bfloat16)

    def columns_of(tile):
        return pl.ds(pl.multiple_of(tile * TILE, TILE), TILE)

    def tile_copy(tile):
        span = columns_of(tile)
        return pltpu.make_async_copy(
            weights_ref.at[0, :, span], own.at[:, span], tile_load.at[tile]
        )

    def hidden_copy(step):
        return pltpu.make_async_copy(hidden_ref.at[0, step], rows_in.at[step], load.at[step, 0])

    def target_copy(step):
        return pltpu.make_async_copy(targets_ref.at[0, step], goal.at[step], load.at[step, 1])

    hidden_copy(0).start()
    for tile in range(tiles):
        tile_copy(tile).start()
    target_copy(0).start()
    hidden_copy(1).start()
    target_copy(1).start()

    barrier = pltpu.get_barrier_semaphore()
    pl.semaphore_signal(barrier, inc=1, device_id=(far, me), device_id_type=MESH)
    pl.semaphore_signal(barrier, inc=1, device_id=(near, me), device_id_type=MESH)

    @pl.when(me > 0)
    def _():
        pl.semaphore_signal(barrier, inc=1, device_id=(replica, me - 1), device_id_type=MESH)

    @pl.when(me < last)
    def _():
        pl.semaphore_signal(barrier, inc=1, device_id=(replica, me + 1), device_id_type=MESH)

    ends = jnp.where((me == 0) | (me == last), 1, 2)
    pl.semaphore_wait(barrier, 2 + ends)

    def slab_rows(slab):
        return pl.ds(pl.multiple_of(slab * SLAB, SLAB), SLAB)

    def remote(source, target, send, recv, device):
        return pltpu.make_async_remote_copy(
            src_ref=source, dst_ref=target, send_sem=send, recv_sem=recv,
            device_id=device, device_id_type=MESH,
        )

    def early_cargo(slab):
        span = slab_rows(slab)
        return remote(
            weights_ref.at[0, span], far_own.at[span],
            cargo_send.at[slab], cargo_recv.at[slab], (far, me),
        )

    def cargo(slab):
        span = slab_rows(slab)
        return remote(
            own.at[span], far_own.at[span],
            cargo_send.at[slab], cargo_recv.at[slab], (far, me),
        )

    def side(index):
        step, low, high = ((0, 0, early), (1, 0, least), (1, least, most))[index]
        target = far_second if step else far_first
        span = pl.ds(low * SLAB, (high - low) * SLAB)
        return remote(
            hidden_ref.at[0, step, :, span], target.at[:, span],
            side_send.at[index], side_recv.at[index], (far, me),
        )

    for slab in range(early):
        early_cargo(slab).start()
    for index in range(2):
        side(index).start()

    @pl.when(parity == 1)
    def _():
        side(2).start()

    @pl.when(me == 0)
    def _():
        for step in range(2):
            arriving[step, 0] = jnp.zeros(arriving.shape[2:], arriving.dtype)

    @pl.when(me == last)
    def _():
        for step in range(2):
            arriving[step, 1] = jnp.zeros(arriving.shape[2:], arriving.dtype)

    def place(chunk):
        return chunk % tiles, pl.ds(pl.multiple_of((chunk // tiles) * ROWS, ROWS), ROWS)

    def right_copy(step, chunk):
        tile, rows = place(chunk)
        return remote(
            out_right.at[tile, rows], arriving.at[step, 0, tile, rows],
            right_send.at[step], right_recv.at[chunk],
            (replica, lax.rem(me + 1, count)),
        )

    def left_copy(step, chunk):
        tile, rows = place(chunk)
        return remote(
            out_left.at[tile, rows], arriving.at[step, 1, tile, rows],
            left_send.at[step], left_recv.at[chunk],
            (replica, lax.rem(me + count - 1, count)),
        )

    block = ROWS // tiles

    def chain(step):
        lag = tiles - 1 + LAG[step] * jnp.maximum(me, last - me)

        def turn(now, _):
            if step:

                @pl.when((now == YIELD) & (parity == 0))
                def _():
                    pl.semaphore_signal(turn_sem, inc=1, device_id=(near, me), device_id_type=MESH)

            @pl.when(now < chunks)
            def _():
                if step == 0:

                    @pl.when(now < tiles)
                    def _():
                        tile_copy(now).wait()

                tile, rows = place(now)
                terms[tile, rows, :] = factor * jnp.dot(
                    rows_in[step, rows, :], own[:, columns_of(tile)],
                    preferred_element_type=jnp.float32,
                )

            rightward = now - LAG[step] * me

            @pl.when((rightward >= 0) & (rightward < chunks))
            def _():
                @pl.when(me > 0)
                def _():
                    right_copy(step, rightward).wait_recv()

                @pl.when(me < last)
                def _():
                    tile, rows = place(rightward)
                    total = terms[tile, rows, :] + arriving[step, 0, tile, rows, :].astype(jnp.float32)
                    out_right[tile, rows, :] = total.astype(jnp.bfloat16)
                    right_copy(step, rightward).start()

            leftward = now - LAG[step] * (last - me)

            @pl.when((leftward >= 0) & (leftward < chunks))
            def _():
                @pl.when(me < last)
                def _():
                    left_copy(step, leftward).wait_recv()

                @pl.when(me > 0)
                def _():
                    tile, rows = place(leftward)
                    total = terms[tile, rows, :] + arriving[step, 1, tile, rows, :].astype(jnp.float32)
                    out_left[tile, rows, :] = total.astype(jnp.bfloat16)
                    left_copy(step, leftward).start()

            index = now - lag

            @pl.when((index >= 0) & (index < chunks))
            def _():
                @pl.when(index == 0)
                def _():
                    target_copy(step).wait()

                rows = pl.ds(pl.multiple_of(index * block, block), block)
                outputs = jnp.concatenate(
                    [
                        terms[tile, rows, :]
                        + arriving[step, 0, tile, rows, :].astype(jnp.float32)
                        + arriving[step, 1, tile, rows, :].astype(jnp.float32)
                        for tile in range(tiles)
                    ],
                    axis=1,
                )
                grads[step, rows, :] = norm_backward(outputs, goal[step, rows, :], gain_ref[...])

            return 0

        hidden_copy(step).wait()
        if step:

            @pl.when(parity == 1)
            def _():
                pl.semaphore_wait(turn_sem, 1)

        lax.fori_loop(0, chunks + tiles - 1 + LAG[step] * last, turn, 0)

    def drain(step):
        @pl.when(me < last)
        def _():
            remote(
                out_right, arriving.at[step, 0], right_send.at[step], right_recv.at[0],
                (replica, lax.rem(me + 1, count)),
            ).wait_send()

        @pl.when(me > 0)
        def _():
            remote(
                out_left, arriving.at[step, 1], left_send.at[step], left_recv.at[0],
                (replica, lax.rem(me + count - 1, count)),
            ).wait_send()

    part = tokens // count

    def part_rows(index):
        return pl.ds(pl.multiple_of(index * part, part), part)

    def across(step):
        return remote(
            grads.at[step, part_rows(me)], far_grads.at[step, part_rows(me)],
            across_send.at[step], across_recv.at[step], (far, me),
        )

    def pass_right(step, index):
        piece = far_grads.at[step, part_rows(index)]
        return remote(
            piece, piece, share_right.at[step, index], share_recv.at[step, index],
            (replica, lax.rem(me + 1, count)),
        )

    def pass_left(step, index):
        piece = far_grads.at[step, part_rows(index)]
        return remote(
            piece, piece, share_left.at[step, index], share_recv.at[step, index],
            (replica, lax.rem(me + count - 1, count)),
        )

    def gather_first(step):
        across(step).wait_recv()

        @pl.when(me < last)
        def _():
            pass_right(step, me).start()

        @pl.when(me > 0)
        def _():
            pass_left(step, me).start()

    def gather_rest(step, low, high):
        def hop(distance, _):
            lower, upper = me - distance, me + distance

            @pl.when(lower >= 0)
            def _():
                pass_right(step, lower).wait_recv()

                @pl.when(me < last)
                def _():
                    pass_right(step, lower).start()

            @pl.when(upper <= last)
            def _():
                pass_left(step, upper).wait_recv()

                @pl.when(me > 0)
                def _():
                    pass_left(step, upper).start()

            return 0

        lax.fori_loop(low, high, hop, 0)

    def gather_sent(step):
        def hop(index, _):
            @pl.when((me < last) & (index <= me))
            def _():
                pass_right(step, index).wait_send()

            @pl.when((me > 0) & (index >= me))
            def _():
                pass_left(step, index).wait_send()

            return 0

        lax.fori_loop(0, count, hop, 0)

    def descended(block_rows, hidden_columns, gradient):
        grad_weight = (factor * contract_rows(hidden_columns, gradient)).astype(jnp.bfloat16)
        return (
            block_rows.astype(jnp.float32) - learn_rate * grad_weight.astype(jnp.float32)
        ).astype(jnp.bfloat16)

    def descend_own(step, span):
        own[span, :] = descended(own[span, :], rows_in[step, :, span], grads[step])

    def pair_rows(pair):
        return pl.ds(pl.multiple_of(pair * PAIR * SLAB, PAIR * SLAB), PAIR * SLAB)

    def near_copy(pair):
        span = pair_rows(pair)
        return remote(
            own.at[span], theirs.at[span], near_send.at[pair], near_recv.at[pair], (near, me)
        )

    def swap(slab):
        span = slab_rows(slab)
        return remote(
            far_own.at[span], crossed.at[span], swap_send.at[slab], swap_recv.at[slab], (near, me)
        )

    def loop(low, high, body):
        def run(index, _):
            body(index)
            return 0

        lax.fori_loop(low, high, run, 0)

    chain(0)
    across(0).start()

    def offer(pair):
        descend_own(0, pair_rows(pair))
        near_copy(pair).start()

    def settle(pair):
        span = pair_rows(pair)
        near_copy(pair).wait()
        own[span, :] = mix(own_mix, own[span, :], theirs[span, :])
        for index in range(PAIR):
            slab = pair * PAIR + index

            @pl.when((slab >= early) & (slab < ready))
            def _():
                cargo(slab).start()

    loop(0, slabs // PAIR, offer)
    loop(0, slabs // PAIR, settle)
    drain(0)

    chain(1)
    across(1).start()
    gather_first(0)

    def give(slab):
        descend_own(1, slab_rows(slab))
        cargo(slab).start()

    loop(ready, slabs, give)
    gather_rest(0, 1, 2)
    gather_first(1)
    gather_rest(0, 2, count)

    def keep(slab):
        @pl.when(slab >= early)
        def _():
            cargo(slab).wait_send()

        descend_own(1, slab_rows(slab))

    loop(0, ready, keep)

    side(0).wait_recv()

    def replay(slab):
        span = slab_rows(slab)
        early_cargo(slab).wait_recv()
        far_own[span, :] = descended(
            far_own[span, :], far_first[:, span], far_grads[0]
        )
        swap(slab).start()

    def level(slab):
        span = slab_rows(slab)
        swap(slab).wait()
        far_own[span, :] = mix(far_mix, far_own[span, :], crossed[span, :])

    loop(0, early, replay)
    loop(0, early, level)
    gather_rest(1, 1, count)
    side(1).wait_recv()

    @pl.when(parity == 1)
    def _():
        side(2).wait_recv()

    def join(slab):
        span = slab_rows(slab)

        @pl.when(slab >= early)
        def _():
            cargo(slab).wait_recv()

        other = descended(far_own[span, :], far_second[:, span], far_grads[1])
        own[span, :] = mix(end_mix, own[span, :], other)

    loop(0, ready, join)

    def finish(slab):
        span = slab_rows(slab)
        cargo(slab).wait()
        own[span, :] = mix(end_mix, own[span, :], far_own[span, :])

    loop(ready, slabs, finish)

    drain(1)
    for step in range(2):
        gather_sent(step)
        across(step).wait_send()
        side(step).wait_send()

    @pl.when(parity == 1)
    def _():
        side(2).wait_send()

    for slab in range(early):
        early_cargo(slab).wait_send()


def on_device(weights, hidden, targets, norm_gain, stragglers):
    _, depth, features = weights.shape
    tokens = hidden.shape[2]
    count = lax.axis_size("tensor")
    tiles = features // TILE
    chunks = tiles * (tokens // ROWS)
    slabs = depth // SLAB
    early = round(slabs * EARLY)
    middles = [round(slabs * part) for part in MIDDLE]
    anywhere = pl.BlockSpec(memory_space=pl.ANY)

    def buffer(*shape, dtype=jnp.bfloat16):
        return pltpu.VMEM(shape, dtype)

    def sems(*shape):
        return pltpu.SemaphoreType.DMA(shape)

    return pl.pallas_call(
        functools.partial(steps_kernel, early, middles),
        out_shape=pltpu.VMEM((depth, features), weights.dtype),
        in_specs=[anywhere] * 3
        + [pl.BlockSpec(memory_space=pltpu.VMEM), pl.BlockSpec(memory_space=pltpu.SMEM)],
        out_specs=pl.BlockSpec(memory_space=pltpu.VMEM),
        scratch_shapes=[
            buffer(depth, features),
            buffer(depth, features),
            buffer(early * SLAB, features),
            buffer(2, tokens, depth),
            buffer(tokens, early * SLAB),
            buffer(tokens, (early + middles[1]) * SLAB),
            buffer(2, tokens, features),
            buffer(tiles, tokens, TILE, dtype=jnp.float32),
            buffer(2, 2, tiles, tokens, TILE),
            buffer(tiles, tokens, TILE),
            buffer(tiles, tokens, TILE),
            buffer(2, tokens, features),
            buffer(2, tokens, features),
            sems(tiles),
            sems(2, 2),
            sems(2),
            sems(chunks),
            sems(2),
            sems(chunks),
            *[sems(slabs // PAIR)] * 2,
            *[sems(slabs)] * 2,
            *[sems(early)] * 2,
            *[sems(3)] * 2,
            *[sems(2)] * 2,
            *[sems(2, count)] * 3,
            pltpu.SemaphoreType.REGULAR,
        ],
        compiler_params=pltpu.CompilerParams(
            collective_id=0, has_side_effects=True, vmem_limit_bytes=56 << 20
        ),
    )(weights, hidden, targets, norm_gain[None], stragglers)[None]


def solution(mesh):
    placed = (
        P("replica", "tensor", None),
        P("replica", None, None, "tensor"),
        P("replica", None, None, None),
        P(),
        P(),
    )
    return jax.shard_map(
        on_device,
        mesh=mesh,
        in_specs=placed,
        out_specs=P("replica", "tensor", None),
        check_vma=False,
    )
```

```python
import functools

import jax
import jax.numpy as jnp
from jax import lax
from jax.experimental import pallas as pl
from jax.experimental.pallas import tpu as pltpu
from jax.sharding import PartitionSpec as P

eps = 1e-05
learn_rate = 0.5

MESH = pl.DeviceIdType.MESH
TILE = 512
ROWS = 64
LAG = (3, 5)
SLAB = 128
PAIR = 2
EARLY = 3 / 14
MIDDLE = (0 / 14, 6 / 14)
YIELD = 36
GROUP = 2
RING = 16
DELAY = 2


def contract_rows(left, right):
    return lax.dot_general(
        left, right, (((0,), (0,)), ((), ())), preferred_element_type=jnp.float32
    )


def norm_backward(outputs, target_rows, norm_gain):
    squares = jnp.mean(outputs * outputs, axis=-1, keepdims=True)
    inverse = lax.rsqrt(squares + eps)
    normed = outputs * inverse
    weighted = (normed * norm_gain - target_rows.astype(jnp.float32)) * norm_gain
    cross_mean = jnp.mean(weighted * normed, axis=-1, keepdims=True)
    return (inverse * (weighted - normed * cross_mean)).astype(jnp.bfloat16)


def flip(index, bit):
    return index + bit - 2 * bit * ((index // bit) % 2)


def steps_kernel(early, middles, *refs):
    weights_ref, hidden_ref, targets_ref, gain_any, late_any, own = refs[:6]
    theirs, far_own, crossed, rows_in, far_first, far_second = refs[6:12]
    goal, terms, arriving, out_right, out_left, grads, far_grads = refs[12:19]
    tile_load, load, right_send, right_recv, left_send, left_recv = refs[19:25]
    near_send, near_recv, cargo_send, cargo_recv, swap_send, swap_recv = refs[25:31]
    side_send, side_recv, across_send, across_recv = refs[31:35]
    share_right, share_left, share_recv, turn_sem, gain_ref, late_ref, small = refs[35:]

    count = lax.axis_size("tensor")
    me = lax.axis_index("tensor")
    replica = lax.axis_index("replica")
    last = count - 1
    near, far = flip(replica, 1), flip(replica, 2)
    cross = flip(near, 2)
    depth, features = own.shape
    tokens = grads.shape[1]
    tiles = terms.shape[0]
    blocks = tokens // ROWS
    chunks = tiles * blocks
    slabs = depth // SLAB
    parity = replica % 2
    least, most = early + middles[0], early + middles[1]
    ready = least + (most - least) * parity
    factor = (depth * count) ** (-0.5)

    def share_of(step, one, other):
        late = (late_ref[step, one] != 0) | (late_ref[step, other] != 0)
        return jnp.where(late, 1.0, 0.5), jnp.where(late, 0.0, 0.5)

    def mix(shares, one, other):
        return (
            one.astype(jnp.float32) * shares[0] + other.astype(jnp.float32) * shares[1]
        ).astype(jnp.bfloat16)

    def columns_of(tile):
        return pl.ds(pl.multiple_of(tile * TILE, TILE), TILE)

    def tile_copy(tile):
        span = columns_of(tile)
        return pltpu.make_async_copy(
            weights_ref.at[0, :, span], own.at[:, span], tile_load.at[tile]
        )

    def hidden_copy(step):
        return pltpu.make_async_copy(hidden_ref.at[0, step], rows_in.at[step], load.at[step, 0])

    def target_copy(step):
        return pltpu.make_async_copy(targets_ref.at[0, step], goal.at[step], load.at[step, 1])

    barrier = pltpu.get_barrier_semaphore()
    pl.semaphore_signal(barrier, inc=1, device_id=(far, me), device_id_type=MESH)
    pl.semaphore_signal(barrier, inc=1, device_id=(near, me), device_id_type=MESH)

    @pl.when(me > 0)
    def _():
        pl.semaphore_signal(barrier, inc=1, device_id=(replica, me - 1), device_id_type=MESH)

    @pl.when(me < last)
    def _():
        pl.semaphore_signal(barrier, inc=1, device_id=(replica, me + 1), device_id_type=MESH)

    gain_copy = pltpu.make_async_copy(gain_any, gain_ref, small.at[0])
    late_copy = pltpu.make_async_copy(late_any, late_ref, small.at[1])
    hidden_copy(0).start()
    for tile in range(tiles):
        tile_copy(tile).start()
    target_copy(0).start()
    gain_copy.start()
    late_copy.start()
    hidden_copy(1).start()
    target_copy(1).start()

    @pl.when(me == 0)
    def _():
        for step in range(2):
            arriving[step, 0] = jnp.zeros(arriving.shape[2:], arriving.dtype)

    @pl.when(me == last)
    def _():
        for step in range(2):
            arriving[step, 1] = jnp.zeros(arriving.shape[2:], arriving.dtype)

    ends = jnp.where((me == 0) | (me == last), 1, 2)
    pl.semaphore_wait(barrier, 2 + ends)

    def slab_rows(slab):
        return pl.ds(pl.multiple_of(slab * SLAB, SLAB), SLAB)

    def remote(source, target, send, recv, device):
        return pltpu.make_async_remote_copy(
            src_ref=source, dst_ref=target, send_sem=send, recv_sem=recv,
            device_id=device, device_id_type=MESH,
        )

    def early_cargo(slab):
        span = slab_rows(slab)
        return remote(
            weights_ref.at[0, span], far_own.at[span],
            cargo_send.at[slab], cargo_recv.at[slab], (far, me),
        )

    def cargo(slab):
        span = slab_rows(slab)
        return remote(
            own.at[span], far_own.at[span],
            cargo_send.at[slab], cargo_recv.at[slab], (far, me),
        )

    def side(index):
        step, low, high = ((0, 0, early), (1, 0, least), (1, least, most))[index]
        target = far_second if step else far_first
        span = pl.ds(low * SLAB, (high - low) * SLAB)
        return remote(
            hidden_ref.at[0, step, :, span], target.at[:, span],
            side_send.at[index], side_recv.at[index], (far, me),
        )

    for slab in range(early):
        early_cargo(slab).start()
    for index in range(2):
        side(index).start()

    @pl.when(parity == 1)
    def _():
        side(2).start()

    def place(chunk):
        return chunk % tiles, pl.ds(pl.multiple_of((chunk // tiles) * ROWS, ROWS), ROWS)

    def right_copy(step, chunk):
        tile, rows = place(chunk)
        return remote(
            out_right.at[tile, rows], arriving.at[step, 0, tile, rows],
            right_send.at[step], right_recv.at[chunk % RING],
            (replica, lax.rem(me + 1, count)),
        )

    def left_copy(step, chunk):
        tile, rows = place(chunk)
        return remote(
            out_left.at[tile, rows], arriving.at[step, 1, tile, rows],
            left_send.at[step], left_recv.at[chunk % RING],
            (replica, lax.rem(me + count - 1, count)),
        )

    block = ROWS // tiles

    def chain(step):
        lag = tiles - 1 + LAG[step] * jnp.maximum(me, last - me)

        def turn(now, _):
            if step:

                @pl.when((now == YIELD) & (parity == 0))
                def _():
                    pl.semaphore_signal(turn_sem, inc=1, device_id=(near, me), device_id_type=MESH)

            @pl.when((now < chunks) & ((now // tiles) % GROUP == 0))
            def _():
                if step == 0:

                    @pl.when(now < tiles)
                    def _():
                        tile_copy(now).wait()

                tile = now % tiles
                rows = pl.ds(pl.multiple_of((now // tiles) * ROWS, GROUP * ROWS), GROUP * ROWS)
                terms[tile, rows, :] = factor * jnp.dot(
                    rows_in[step, rows, :], own[:, columns_of(tile)],
                    preferred_element_type=jnp.float32,
                )

            rightward = now - LAG[step] * me

            @pl.when((rightward >= 0) & (rightward < chunks))
            def _():
                @pl.when(me > 0)
                def _():
                    right_copy(step, rightward).wait_recv()

                @pl.when(me < last)
                def _():
                    tile, rows = place(rightward)
                    total = terms[tile, rows, :] + arriving[step, 0, tile, rows, :].astype(jnp.float32)
                    out_right[tile, rows, :] = total.astype(jnp.bfloat16)
                    right_copy(step, rightward).start()

            leftward = now - LAG[step] * (last - me)

            @pl.when((leftward >= 0) & (leftward < chunks))
            def _():
                @pl.when(me < last)
                def _():
                    left_copy(step, leftward).wait_recv()

                @pl.when(me > 0)
                def _():
                    tile, rows = place(leftward)
                    total = terms[tile, rows, :] + arriving[step, 1, tile, rows, :].astype(jnp.float32)
                    out_left[tile, rows, :] = total.astype(jnp.bfloat16)
                    left_copy(step, leftward).start()

            index = now - lag

            @pl.when((index >= 0) & (index < chunks))
            def _():
                @pl.when(index == 0)
                def _():
                    target_copy(step).wait()
                    if step == 0:
                        gain_copy.wait()

                rows = pl.ds(pl.multiple_of(index * block, block), block)
                outputs = jnp.concatenate(
                    [
                        terms[tile, rows, :]
                        + arriving[step, 0, tile, rows, :].astype(jnp.float32)
                        + arriving[step, 1, tile, rows, :].astype(jnp.float32)
                        for tile in range(tiles)
                    ],
                    axis=1,
                )
                grads[step, rows, :] = norm_backward(outputs, goal[step, rows, :], gain_ref[...])

            return 0

        hidden_copy(step).wait()
        if step:

            @pl.when(parity == 1)
            def _():
                pl.semaphore_wait(turn_sem, 1)

        lax.fori_loop(0, chunks + tiles - 1 + LAG[step] * last, turn, 0)

    def drain(step):
        @pl.when(me < last)
        def _():
            remote(
                out_right, arriving.at[step, 0], right_send.at[step], right_recv.at[0],
                (replica, lax.rem(me + 1, count)),
            ).wait_send()

        @pl.when(me > 0)
        def _():
            remote(
                out_left, arriving.at[step, 1], left_send.at[step], left_recv.at[0],
                (replica, lax.rem(me + count - 1, count)),
            ).wait_send()

    part = tokens // count

    def part_rows(index):
        return pl.ds(pl.multiple_of(index * part, part), part)

    def across(step):
        return remote(
            grads.at[step, part_rows(me)], far_grads.at[step, part_rows(me)],
            across_send.at[step], across_recv.at[step], (far, me),
        )

    def pass_right(step, index):
        piece = far_grads.at[step, part_rows(index)]
        return remote(
            piece, piece, share_right.at[step, index], share_recv.at[step, index],
            (replica, lax.rem(me + 1, count)),
        )

    def pass_left(step, index):
        piece = far_grads.at[step, part_rows(index)]
        return remote(
            piece, piece, share_left.at[step, index], share_recv.at[step, index],
            (replica, lax.rem(me + count - 1, count)),
        )

    def gather_first(step):
        across(step).wait_recv()

        @pl.when(me < last)
        def _():
            pass_right(step, me).start()

        @pl.when(me > 0)
        def _():
            pass_left(step, me).start()

    def gather_rest(step, low, high):
        def hop(distance, _):
            lower, upper = me - distance, me + distance

            @pl.when(lower >= 0)
            def _():
                pass_right(step, lower).wait_recv()

                @pl.when(me < last)
                def _():
                    pass_right(step, lower).start()

            @pl.when(upper <= last)
            def _():
                pass_left(step, upper).wait_recv()

                @pl.when(me > 0)
                def _():
                    pass_left(step, upper).start()

            return 0

        lax.fori_loop(low, high, hop, 0)

    def gather_sent(step):
        def hop(index, _):
            @pl.when((me < last) & (index <= me))
            def _():
                pass_right(step, index).wait_send()

            @pl.when((me > 0) & (index >= me))
            def _():
                pass_left(step, index).wait_send()

            return 0

        lax.fori_loop(0, count, hop, 0)

    def descended(block_rows, hidden_columns, gradient):
        grad_weight = (factor * contract_rows(hidden_columns, gradient)).astype(jnp.bfloat16)
        return (
            block_rows.astype(jnp.float32) - learn_rate * grad_weight.astype(jnp.float32)
        ).astype(jnp.bfloat16)

    def descend_own(step, span):
        own[span, :] = descended(own[span, :], rows_in[step, :, span], grads[step])

    def pair_rows(pair):
        return pl.ds(pl.multiple_of(pair * PAIR * SLAB, PAIR * SLAB), PAIR * SLAB)

    def near_copy(pair):
        span = pair_rows(pair)
        return remote(
            own.at[span], theirs.at[span], near_send.at[pair], near_recv.at[pair], (near, me)
        )

    def swap(slab):
        span = slab_rows(slab)
        return remote(
            far_own.at[span], crossed.at[span], swap_send.at[slab], swap_recv.at[slab], (near, me)
        )

    def loop(low, high, body):
        def run(index, _):
            body(index)
            return 0

        lax.fori_loop(low, high, run, 0)

    chain(0)
    across(0).start()
    late_copy.wait()
    own_mix = share_of(0, replica, near)
    far_mix = share_of(0, far, cross)
    end_mix = share_of(1, replica, far)

    def offer(pair):
        descend_own(0, pair_rows(pair))
        near_copy(pair).start()

    def settle(pair):
        span = pair_rows(pair)
        near_copy(pair).wait()
        own[span, :] = mix(own_mix, own[span, :], theirs[span, :])
        for index in range(PAIR):
            slab = pair * PAIR + index

            @pl.when((slab >= early) & (slab < ready))
            def _():
                cargo(slab).start()

    def trade(pair):
        @pl.when(pair < slabs // PAIR)
        def _():
            offer(pair)

        @pl.when(pair >= DELAY)
        def _():
            settle(pair - DELAY)

    loop(0, slabs // PAIR + DELAY, trade)
    drain(0)

    chain(1)
    across(1).start()
    gather_first(0)

    def give(slab):
        descend_own(1, slab_rows(slab))
        cargo(slab).start()

    loop(ready, slabs, give)
    gather_rest(0, 1, 2)
    gather_first(1)
    gather_rest(0, 2, count)

    def keep(slab):
        @pl.when(slab >= early)
        def _():
            cargo(slab).wait_send()

        descend_own(1, slab_rows(slab))

    loop(0, ready, keep)

    side(0).wait_recv()

    def replay(slab):
        span = slab_rows(slab)
        early_cargo(slab).wait_recv()
        far_own[span, :] = descended(
            far_own[span, :], far_first[:, span], far_grads[0]
        )
        swap(slab).start()

    def level(slab):
        span = slab_rows(slab)
        swap(slab).wait()
        far_own[span, :] = mix(far_mix, far_own[span, :], crossed[span, :])

    loop(0, early, replay)
    loop(0, early, level)
    gather_rest(1, 1, count)
    side(1).wait_recv()

    @pl.when(parity == 1)
    def _():
        side(2).wait_recv()

    def join(slab):
        span = slab_rows(slab)

        @pl.when(slab >= early)
        def _():
            cargo(slab).wait_recv()

        other = descended(far_own[span, :], far_second[:, span], far_grads[1])
        own[span, :] = mix(end_mix, own[span, :], other)

    loop(0, ready, join)

    def finish(slab):
        span = slab_rows(slab)
        cargo(slab).wait()
        own[span, :] = mix(end_mix, own[span, :], far_own[span, :])

    loop(ready, slabs, finish)

    drain(1)
    for step in range(2):
        gather_sent(step)
        across(step).wait_send()
        side(step).wait_send()

    @pl.when(parity == 1)
    def _():
        side(2).wait_send()

    for slab in range(early):
        early_cargo(slab).wait_send()


def on_device(weights, hidden, targets, norm_gain, stragglers):
    _, depth, features = weights.shape
    tokens = hidden.shape[2]
    count = lax.axis_size("tensor")
    tiles = features // TILE
    chunks = tiles * (tokens // ROWS)
    slabs = depth // SLAB
    early = round(slabs * EARLY)
    middles = [round(slabs * part) for part in MIDDLE]
    anywhere = pl.BlockSpec(memory_space=pl.ANY)

    def buffer(*shape, dtype=jnp.bfloat16):
        return pltpu.VMEM(shape, dtype)

    def sems(*shape):
        return pltpu.SemaphoreType.DMA(shape)

    return pl.pallas_call(
        functools.partial(steps_kernel, early, middles),
        out_shape=pltpu.VMEM((depth, features), weights.dtype),
        in_specs=[anywhere] * 5,
        out_specs=pl.BlockSpec(memory_space=pltpu.VMEM),
        scratch_shapes=[
            buffer(depth, features),
            buffer(depth, features),
            buffer(early * SLAB, features),
            buffer(2, tokens, depth),
            buffer(tokens, early * SLAB),
            buffer(tokens, (early + middles[1]) * SLAB),
            buffer(2, tokens, features),
            buffer(tiles, tokens, TILE, dtype=jnp.float32),
            buffer(2, 2, tiles, tokens, TILE),
            buffer(tiles, tokens, TILE),
            buffer(tiles, tokens, TILE),
            buffer(2, tokens, features),
            buffer(2, tokens, features),
            sems(tiles),
            sems(2, 2),
            sems(2),
            sems(RING),
            sems(2),
            sems(RING),
            *[sems(slabs // PAIR)] * 2,
            *[sems(slabs)] * 2,
            *[sems(early)] * 2,
            *[sems(3)] * 2,
            *[sems(2)] * 2,
            *[sems(2, count)] * 3,
            pltpu.SemaphoreType.REGULAR,
            buffer(1, features, dtype=jnp.float32),
            pltpu.SMEM(stragglers.shape, stragglers.dtype),
            sems(2),
        ],
        compiler_params=pltpu.CompilerParams(
            collective_id=0, has_side_effects=True, vmem_limit_bytes=56 << 20
        ),
    )(weights, hidden, targets, norm_gain[None], stragglers)[None]


def solution(mesh):
    placed = (
        P("replica", "tensor", None),
        P("replica", None, None, "tensor"),
        P("replica", None, None, None),
        P(),
        P(),
    )
    return jax.shard_map(
        on_device,
        mesh=mesh,
        in_specs=placed,
        out_specs=P("replica", "tensor", None),
        check_vma=False,
    )
```

```python
import functools

import jax
import jax.numpy as jnp
from jax import lax
from jax.experimental import pallas as pl
from jax.experimental.pallas import tpu as pltpu
from jax.sharding import PartitionSpec as P

eps = 1e-05
learn_rate = 0.5

MESH = pl.DeviceIdType.MESH
TILE = 512
ROWS = 64
LAG = (3, 5)
SLAB = 128
PAIR = 2
EARLY = 3 / 14
MIDDLE = (2 / 14, 4 / 14)
YIELD = 36
GROUP = 2
RING = 16
DELAY = 2


def contract_rows(left, right):
    return lax.dot_general(
        left, right, (((0,), (0,)), ((), ())), preferred_element_type=jnp.float32
    )


def norm_backward(outputs, target_rows, norm_gain):
    squares = jnp.mean(outputs * outputs, axis=-1, keepdims=True)
    inverse = lax.rsqrt(squares + eps)
    normed = outputs * inverse
    weighted = (normed * norm_gain - target_rows.astype(jnp.float32)) * norm_gain
    cross_mean = jnp.mean(weighted * normed, axis=-1, keepdims=True)
    return (inverse * (weighted - normed * cross_mean)).astype(jnp.bfloat16)


def flip(index, bit):
    return index + bit - 2 * bit * ((index // bit) % 2)


def steps_kernel(early, middles, *refs):
    weights_ref, hidden_ref, targets_ref, gain_any, late_any, own = refs[:6]
    theirs, far_own, crossed, rows_in, far_first, far_second = refs[6:12]
    goal, terms, arriving, out_right, out_left, grads, far_grads = refs[12:19]
    tile_load, load, right_send, right_recv, left_send, left_recv = refs[19:25]
    near_send, near_recv, cargo_send, cargo_recv, swap_send, swap_recv = refs[25:31]
    side_send, side_recv, across_send, across_recv = refs[31:35]
    share_right, share_left, share_recv, turn_sem, gain_ref, late_ref, small = refs[35:]

    count = lax.axis_size("tensor")
    me = lax.axis_index("tensor")
    replica = lax.axis_index("replica")
    last = count - 1
    near, far = flip(replica, 1), flip(replica, 2)
    cross = flip(near, 2)
    depth, features = own.shape
    tokens = grads.shape[1]
    tiles = terms.shape[0]
    blocks = tokens // ROWS
    chunks = tiles * blocks
    slabs = depth // SLAB
    parity = replica % 2
    least, most = early + middles[0], early + middles[1]
    ready = least + (most - least) * parity
    factor = (depth * count) ** (-0.5)

    def share_of(step, one, other):
        late = (late_ref[step, one] != 0) | (late_ref[step, other] != 0)
        return jnp.where(late, 1.0, 0.5), jnp.where(late, 0.0, 0.5)

    def mix(shares, one, other):
        return (
            one.astype(jnp.float32) * shares[0] + other.astype(jnp.float32) * shares[1]
        ).astype(jnp.bfloat16)

    def columns_of(tile):
        return pl.ds(pl.multiple_of(tile * TILE, TILE), TILE)

    def tile_copy(tile):
        span = columns_of(tile)
        return pltpu.make_async_copy(
            weights_ref.at[0, :, span], own.at[:, span], tile_load.at[tile]
        )

    def hidden_copy(step):
        return pltpu.make_async_copy(hidden_ref.at[0, step], rows_in.at[step], load.at[step, 0])

    def target_copy(step):
        return pltpu.make_async_copy(targets_ref.at[0, step], goal.at[step], load.at[step, 1])

    barrier = pltpu.get_barrier_semaphore()
    pl.semaphore_signal(barrier, inc=1, device_id=(far, me), device_id_type=MESH)
    pl.semaphore_signal(barrier, inc=1, device_id=(near, me), device_id_type=MESH)

    @pl.when(me > 0)
    def _():
        pl.semaphore_signal(barrier, inc=1, device_id=(replica, me - 1), device_id_type=MESH)

    @pl.when(me < last)
    def _():
        pl.semaphore_signal(barrier, inc=1, device_id=(replica, me + 1), device_id_type=MESH)

    gain_copy = pltpu.make_async_copy(gain_any, gain_ref, small.at[0])
    late_copy = pltpu.make_async_copy(late_any, late_ref, small.at[1])
    hidden_copy(0).start()
    for tile in range(tiles):
        tile_copy(tile).start()
    target_copy(0).start()
    gain_copy.start()
    late_copy.start()
    hidden_copy(1).start()
    target_copy(1).start()

    @pl.when(me == 0)
    def _():
        for step in range(2):
            arriving[step, 0] = jnp.zeros(arriving.shape[2:], arriving.dtype)

    @pl.when(me == last)
    def _():
        for step in range(2):
            arriving[step, 1] = jnp.zeros(arriving.shape[2:], arriving.dtype)

    ends = jnp.where((me == 0) | (me == last), 1, 2)
    pl.semaphore_wait(barrier, 2 + ends)

    def slab_rows(slab):
        return pl.ds(pl.multiple_of(slab * SLAB, SLAB), SLAB)

    def remote(source, target, send, recv, device):
        return pltpu.make_async_remote_copy(
            src_ref=source, dst_ref=target, send_sem=send, recv_sem=recv,
            device_id=device, device_id_type=MESH,
        )

    def early_cargo(slab):
        span = slab_rows(slab)
        return remote(
            weights_ref.at[0, span], far_own.at[span],
            cargo_send.at[slab], cargo_recv.at[slab], (far, me),
        )

    def cargo(slab):
        span = slab_rows(slab)
        return remote(
            own.at[span], far_own.at[span],
            cargo_send.at[slab], cargo_recv.at[slab], (far, me),
        )

    def side(index):
        step, low, high = ((0, 0, early), (1, 0, least), (1, least, most))[index]
        target = far_second if step else far_first
        span = pl.ds(low * SLAB, (high - low) * SLAB)
        return remote(
            hidden_ref.at[0, step, :, span], target.at[:, span],
            side_send.at[index], side_recv.at[index], (far, me),
        )

    for slab in range(early):
        early_cargo(slab).start()
    for index in range(2):
        side(index).start()

    @pl.when(parity == 1)
    def _():
        side(2).start()

    def place(chunk):
        return chunk % tiles, pl.ds(pl.multiple_of((chunk // tiles) * ROWS, ROWS), ROWS)

    def right_copy(step, chunk):
        tile, rows = place(chunk)
        return remote(
            out_right.at[tile, rows], arriving.at[step, 0, tile, rows],
            right_send.at[step], right_recv.at[chunk % RING],
            (replica, lax.rem(me + 1, count)),
        )

    def left_copy(step, chunk):
        tile, rows = place(chunk)
        return remote(
            out_left.at[tile, rows], arriving.at[step, 1, tile, rows],
            left_send.at[step], left_recv.at[chunk % RING],
            (replica, lax.rem(me + count - 1, count)),
        )

    block = ROWS // tiles

    def chain(step):
        lag = tiles - 1 + LAG[step] * jnp.maximum(me, last - me)

        def turn(now, _):
            if step:

                @pl.when((now == YIELD) & (parity == 0))
                def _():
                    pl.semaphore_signal(turn_sem, inc=1, device_id=(near, me), device_id_type=MESH)

            @pl.when((now < chunks) & ((now // tiles) % GROUP == 0))
            def _():
                if step == 0:

                    @pl.when(now < tiles)
                    def _():
                        tile_copy(now).wait()

                tile = now % tiles
                rows = pl.ds(pl.multiple_of((now // tiles) * ROWS, GROUP * ROWS), GROUP * ROWS)
                terms[tile, rows, :] = factor * jnp.dot(
                    rows_in[step, rows, :], own[:, columns_of(tile)],
                    preferred_element_type=jnp.float32,
                )

            rightward = now - LAG[step] * me

            @pl.when((rightward >= 0) & (rightward < chunks))
            def _():
                @pl.when(me > 0)
                def _():
                    right_copy(step, rightward).wait_recv()

                @pl.when(me < last)
                def _():
                    tile, rows = place(rightward)
                    total = terms[tile, rows, :] + arriving[step, 0, tile, rows, :].astype(jnp.float32)
                    out_right[tile, rows, :] = total.astype(jnp.bfloat16)
                    right_copy(step, rightward).start()

            leftward = now - LAG[step] * (last - me)

            @pl.when((leftward >= 0) & (leftward < chunks))
            def _():
                @pl.when(me < last)
                def _():
                    left_copy(step, leftward).wait_recv()

                @pl.when(me > 0)
                def _():
                    tile, rows = place(leftward)
                    total = terms[tile, rows, :] + arriving[step, 1, tile, rows, :].astype(jnp.float32)
                    out_left[tile, rows, :] = total.astype(jnp.bfloat16)
                    left_copy(step, leftward).start()

            index = now - lag

            @pl.when((index >= 0) & (index < chunks))
            def _():
                @pl.when(index == 0)
                def _():
                    target_copy(step).wait()
                    if step == 0:
                        gain_copy.wait()

                rows = pl.ds(pl.multiple_of(index * block, block), block)
                outputs = jnp.concatenate(
                    [
                        terms[tile, rows, :]
                        + arriving[step, 0, tile, rows, :].astype(jnp.float32)
                        + arriving[step, 1, tile, rows, :].astype(jnp.float32)
                        for tile in range(tiles)
                    ],
                    axis=1,
                )
                grads[step, rows, :] = norm_backward(outputs, goal[step, rows, :], gain_ref[...])

            return 0

        hidden_copy(step).wait()
        if step:

            @pl.when(parity == 1)
            def _():
                pl.semaphore_wait(turn_sem, 1)

        lax.fori_loop(0, chunks + tiles - 1 + LAG[step] * last, turn, 0)

    def drain(step):
        @pl.when(me < last)
        def _():
            remote(
                out_right, arriving.at[step, 0], right_send.at[step], right_recv.at[0],
                (replica, lax.rem(me + 1, count)),
            ).wait_send()

        @pl.when(me > 0)
        def _():
            remote(
                out_left, arriving.at[step, 1], left_send.at[step], left_recv.at[0],
                (replica, lax.rem(me + count - 1, count)),
            ).wait_send()

    part = tokens // count

    def part_rows(index):
        return pl.ds(pl.multiple_of(index * part, part), part)

    def across(step):
        return remote(
            grads.at[step, part_rows(me)], far_grads.at[step, part_rows(me)],
            across_send.at[step], across_recv.at[step], (far, me),
        )

    def pass_right(step, index):
        piece = far_grads.at[step, part_rows(index)]
        return remote(
            piece, piece, share_right.at[step, index], share_recv.at[step, index],
            (replica, lax.rem(me + 1, count)),
        )

    def pass_left(step, index):
        piece = far_grads.at[step, part_rows(index)]
        return remote(
            piece, piece, share_left.at[step, index], share_recv.at[step, index],
            (replica, lax.rem(me + count - 1, count)),
        )

    def gather_first(step):
        across(step).wait_recv()

        @pl.when(me < last)
        def _():
            pass_right(step, me).start()

        @pl.when(me > 0)
        def _():
            pass_left(step, me).start()

    def gather_rest(step, low, high):
        def hop(distance, _):
            lower, upper = me - distance, me + distance

            @pl.when(lower >= 0)
            def _():
                pass_right(step, lower).wait_recv()

                @pl.when(me < last)
                def _():
                    pass_right(step, lower).start()

            @pl.when(upper <= last)
            def _():
                pass_left(step, upper).wait_recv()

                @pl.when(me > 0)
                def _():
                    pass_left(step, upper).start()

            return 0

        lax.fori_loop(low, high, hop, 0)

    def gather_sent(step):
        def hop(index, _):
            @pl.when((me < last) & (index <= me))
            def _():
                pass_right(step, index).wait_send()

            @pl.when((me > 0) & (index >= me))
            def _():
                pass_left(step, index).wait_send()

            return 0

        lax.fori_loop(0, count, hop, 0)

    def descended(block_rows, hidden_columns, gradient):
        grad_weight = (factor * contract_rows(hidden_columns, gradient)).astype(jnp.bfloat16)
        return (
            block_rows.astype(jnp.float32) - learn_rate * grad_weight.astype(jnp.float32)
        ).astype(jnp.bfloat16)

    def descend_own(step, span):
        own[span, :] = descended(own[span, :], rows_in[step, :, span], grads[step])

    def pair_rows(pair):
        return pl.ds(pl.multiple_of(pair * PAIR * SLAB, PAIR * SLAB), PAIR * SLAB)

    def near_copy(pair):
        span = pair_rows(pair)
        return remote(
            own.at[span], theirs.at[span], near_send.at[pair], near_recv.at[pair], (near, me)
        )

    def swap(slab):
        span = slab_rows(slab)
        return remote(
            far_own.at[span], crossed.at[span], swap_send.at[slab], swap_recv.at[slab], (near, me)
        )

    def loop(low, high, body):
        def run(index, _):
            body(index)
            return 0

        lax.fori_loop(low, high, run, 0)

    chain(0)
    across(0).start()
    late_copy.wait()
    own_mix = share_of(0, replica, near)
    far_mix = share_of(0, far, cross)
    end_mix = share_of(1, replica, far)

    def offer(pair):
        descend_own(0, pair_rows(pair))
        near_copy(pair).start()

    def settle(pair):
        span = pair_rows(pair)
        near_copy(pair).wait()
        own[span, :] = mix(own_mix, own[span, :], theirs[span, :])
        for index in range(PAIR):
            slab = pair * PAIR + index

            @pl.when((slab >= early) & (slab < ready))
            def _():
                cargo(slab).start()

    def trade(pair):
        @pl.when(pair < slabs // PAIR)
        def _():
            offer(pair)

        @pl.when(pair >= DELAY)
        def _():
            settle(pair - DELAY)

    loop(0, slabs // PAIR + DELAY, trade)
    drain(0)

    chain(1)
    across(1).start()
    gather_first(0)

    def give(slab):
        descend_own(1, slab_rows(slab))
        cargo(slab).start()

    loop(ready, slabs, give)
    gather_rest(0, 1, 2)
    gather_first(1)
    gather_rest(0, 2, count)

    def keep(slab):
        @pl.when(slab >= early)
        def _():
            cargo(slab).wait_send()

        descend_own(1, slab_rows(slab))

    loop(0, ready, keep)

    side(0).wait_recv()

    def replay(slab):
        span = slab_rows(slab)
        early_cargo(slab).wait_recv()
        far_own[span, :] = descended(
            far_own[span, :], far_first[:, span], far_grads[0]
        )
        swap(slab).start()

    def level(slab):
        span = slab_rows(slab)
        swap(slab).wait()
        far_own[span, :] = mix(far_mix, far_own[span, :], crossed[span, :])

    loop(0, early, replay)
    loop(0, early, level)
    gather_rest(1, 1, count)
    side(1).wait_recv()

    @pl.when(parity == 1)
    def _():
        side(2).wait_recv()

    def join(slab):
        span = slab_rows(slab)

        @pl.when(slab >= early)
        def _():
            cargo(slab).wait_recv()

        other = descended(far_own[span, :], far_second[:, span], far_grads[1])
        own[span, :] = mix(end_mix, own[span, :], other)

    loop(0, ready, join)

    def finish(slab):
        span = slab_rows(slab)
        cargo(slab).wait()
        own[span, :] = mix(end_mix, own[span, :], far_own[span, :])

    loop(ready, slabs, finish)

    drain(1)
    for step in range(2):
        gather_sent(step)
        across(step).wait_send()
        side(step).wait_send()

    @pl.when(parity == 1)
    def _():
        side(2).wait_send()

    for slab in range(early):
        early_cargo(slab).wait_send()


def on_device(weights, hidden, targets, norm_gain, stragglers):
    _, depth, features = weights.shape
    tokens = hidden.shape[2]
    count = lax.axis_size("tensor")
    tiles = features // TILE
    chunks = tiles * (tokens // ROWS)
    slabs = depth // SLAB
    early = round(slabs * EARLY)
    middles = [round(slabs * part) for part in MIDDLE]
    anywhere = pl.BlockSpec(memory_space=pl.ANY)

    def buffer(*shape, dtype=jnp.bfloat16):
        return pltpu.VMEM(shape, dtype)

    def sems(*shape):
        return pltpu.SemaphoreType.DMA(shape)

    return pl.pallas_call(
        functools.partial(steps_kernel, early, middles),
        out_shape=pltpu.VMEM((depth, features), weights.dtype),
        in_specs=[anywhere] * 5,
        out_specs=pl.BlockSpec(memory_space=pltpu.VMEM),
        scratch_shapes=[
            buffer(depth, features),
            buffer(depth, features),
            buffer(early * SLAB, features),
            buffer(2, tokens, depth),
            buffer(tokens, early * SLAB),
            buffer(tokens, (early + middles[1]) * SLAB),
            buffer(2, tokens, features),
            buffer(tiles, tokens, TILE, dtype=jnp.float32),
            buffer(2, 2, tiles, tokens, TILE),
            buffer(tiles, tokens, TILE),
            buffer(tiles, tokens, TILE),
            buffer(2, tokens, features),
            buffer(2, tokens, features),
            sems(tiles),
            sems(2, 2),
            sems(2),
            sems(RING),
            sems(2),
            sems(RING),
            *[sems(slabs // PAIR)] * 2,
            *[sems(slabs)] * 2,
            *[sems(early)] * 2,
            *[sems(3)] * 2,
            *[sems(2)] * 2,
            *[sems(2, count)] * 3,
            pltpu.SemaphoreType.REGULAR,
            buffer(1, features, dtype=jnp.float32),
            pltpu.SMEM(stragglers.shape, stragglers.dtype),
            sems(2),
        ],
        compiler_params=pltpu.CompilerParams(
            collective_id=0, has_side_effects=True, vmem_limit_bytes=56 << 20
        ),
    )(weights, hidden, targets, norm_gain[None], stragglers)[None]


def solution(mesh):
    placed = (
        P("replica", "tensor", None),
        P("replica", None, None, "tensor"),
        P("replica", None, None, None),
        P(),
        P(),
    )
    return jax.shard_map(
        on_device,
        mesh=mesh,
        in_specs=placed,
        out_specs=P("replica", "tensor", None),
        check_vma=False,
    )
```
